512 devices in a mesh: scen: 64 (over y, z), fac: 8 (over x, core).
Axes of the slice: x: 4, y: 8, z: 8, core: 2. Of those that a mesh axis runs over, the one named last changes fastest.
Arguments:
- scenarios: bfloat16 [4096, 8192], P(('scen', 'fac')), may hold values from -40 to 40
Outputs:
- shrunk: float32 [8192, 8192], P('scen', 'fac')
- shrinkage: float32 [], replicated
- col_mean: float32 [8192], P('fac')
The draws below stay inside these ranges and needn't reach their ends.
All inputs are finite; a program needn't handle non-finite values.
Results may differ from the reference program's by a relative error of at most 0.0008.
Values may be sent and summed in bfloat16 or wider, within the bound.
No kernel may reach another device: no remote copies, remote signals or barrier semaphores. Data moves between devices by JAX's collectives and lax.ppermute only.
A program may use at most 64 MiB of HBM per device.

```python
import math
import jax
import jax.numpy as jnp
from jax import lax

FACTORS = 8192
SCENARIOS = 4096


def draw_scenarios(key, part):
    keys = jax.random.split(key, 3)
    offsets = jax.random.uniform(keys[0], (FACTORS,), jnp.float32, -12.0, 12.0)
    position = jnp.arange(SCENARIOS, dtype=jnp.float32) / (SCENARIOS - 1)
    ramp = 0.5 + position
    row_scale = 0.6 + 1.2 * position
    scales = jnp.exp(jax.random.uniform(keys[1], (FACTORS,), jnp.float32, math.log(0.3), math.log(3.0)))
    noise = jnp.clip(jax.random.normal(keys[2], (SCENARIOS, FACTORS), jnp.float32), -4.0, 4.0)
    values = offsets * ramp[:, None] + scales * row_scale[:, None] * noise
    return jnp.clip(values, -40.0, 40.0).astype(jnp.bfloat16)


def setup_inputs(seed: int = 0) -> dict:
    arg_keys = jax.random.split(jax.random.key(seed), 2)
    scenarios = draw_scenarios(jax.random.fold_in(arg_keys[1], 71), 0)
    return dict(scenarios=scenarios)


def reference(scenarios):
    values = scenarios.astype(jnp.float32)
    col_mean = jnp.sum(values, axis=0) / SCENARIOS
    centered = (values - col_mean).astype(jnp.bfloat16)
    as_float = centered.astype(jnp.float32)
    squared = jnp.sum(as_float * as_float, axis=1)
    trace_total = jnp.sum(squared)
    fourth_total = jnp.sum(squared * squared)
    covariance = jnp.dot(as_float.T, as_float, precision=lax.Precision.HIGHEST) / SCENARIOS
    mu_scale = trace_total / (SCENARIOS * FACTORS)
    diag_mask = jnp.eye(FACTORS, dtype=jnp.float32)
    distance = covariance - mu_scale * diag_mask
    spread = jnp.sum(distance * distance) / FACTORS
    norm_sq = FACTORS * (spread + mu_scale * mu_scale)
    beta_value = (fourth_total / SCENARIOS - norm_sq) / (FACTORS * SCENARIOS)
    shrinkage = beta_value / spread
    shrunk = (1.0 - shrinkage) * covariance + shrinkage * mu_scale * diag_mask
    return shrunk, shrinkage, col_mean
```

```python
import jax
import jax.numpy as jnp
from jax import lax
from jax.sharding import Mesh
from jax.sharding import PartitionSpec as P

PLANE = ("y", "z")
LINE = ("x", "c")
SLAB = ("z", "x", "c")
F32 = jnp.float32
BF16 = jnp.bfloat16
EXTRA = 8


def gather_small(row, axes):
    copies = jnp.broadcast_to(row[None], (lax.axis_size(axes), *row.shape))
    return lax.all_to_all(copies, axes, split_axis=0, concat_axis=0, tiled=True)


def partial_rows(left, right):
    return lax.dot_general(left, right, (((0,), (0,)), ((), ())), preferred_element_type=F32)


def on_device(scenarios):
    row_count, factors = scenarios.shape
    ny, nz, nx, nc = (lax.axis_size(axis) for axis in ("y", "z", "x", "c"))
    nf = nx * nc
    total_rows = row_count * ny * nz * nf
    block = factors // ny
    width = block // nf
    y_idx, z_idx, c_idx = lax.axis_index("y"), lax.axis_index("z"), lax.axis_index("c")
    f_idx = lax.axis_index(LINE)

    blocks = scenarios.reshape(row_count, ny, block).transpose(1, 0, 2)
    to_rows = jnp.broadcast_to(blocks[:, None], (ny, nz, row_count, block))
    to_cols = jnp.broadcast_to(blocks[None, :], (ny, nz, row_count, block))
    outgoing = jnp.stack((to_rows, to_cols), axis=2).reshape(ny * nz, 2, row_count, block)
    arrived = lax.all_to_all(outgoing, PLANE, split_axis=0, concat_axis=0, tiled=True)

    part_rows = row_count * ny * nz
    local_mean = jnp.sum(arrived.astype(F32), axis=(0, 2)) / part_rows
    centered = (arrived.astype(F32) - local_mean[None, :, None, :]).astype(BF16)
    left = centered[:, 0].reshape(part_rows, nx, nc, width)
    right = centered[:, 1].reshape(part_rows, block)

    mean_cols = jnp.broadcast_to(local_mean[1], (nx, block))
    mean_rows = local_mean[0].reshape(nx, nc, width)

    def extra_rows(core):
        rows = lax.dynamic_index_in_dim(mean_rows, core, 1, keepdims=False)
        rows = jnp.pad(rows, ((0, 0), (0, block - width)))
        slot = lax.broadcasted_iota(jnp.int32, (nx, EXTRA, block), 1)
        return jnp.where(
            slot == c_idx, mean_cols[:, None], jnp.where(slot == nc + c_idx, rows[:, None], 0.0)
        )

    def half(core):
        picked = lax.dynamic_index_in_dim(left, core, 2, keepdims=False)
        return jnp.concatenate((partial_rows(picked, right), extra_rows(core)), axis=1)

    swapped = lax.ppermute(half(1 - c_idx), "c", [(0, 1), (1, 0)])
    chip_sum = half(c_idx) + swapped
    pieces = lax.all_to_all(chip_sum, "x", split_axis=0, concat_axis=0, tiled=True)

    scatter = jnp.sum(pieces[:, :width], axis=0)
    means_c = pieces[:, width : width + nc].reshape(nf, block)
    means_r = pieces[:, width + nc : width + 2 * nc, :width].reshape(nf, width)
    mean_c = jnp.sum(means_c, axis=0) / nf
    mean_r = jnp.sum(means_r, axis=0) / nf
    off_c = means_c - mean_c
    off_r = means_r - mean_r
    between = jnp.sum(off_r[:, :, None] * off_c[:, None, :], axis=0)
    covariance = (scatter + part_rows * between) / total_rows

    packed = jnp.concatenate(
        (covariance, jnp.broadcast_to(mean_c, (EXTRA, block))), axis=0
    )
    pairs = [(z * nf + f, f * nz + z) for z in range(nz) for f in range(nf)]
    owned = lax.ppermute(packed, SLAB, pairs)

    mine = lax.dynamic_slice_in_dim(arrived, y_idx * nz, nz, 0)[:, 1]
    mine = (mine.astype(F32) - mean_c).astype(BF16).astype(F32)
    norms = jnp.sum(mine * mine, axis=2).reshape(nz * row_count)

    row_at = f_idx * width + lax.broadcasted_iota(jnp.int32, (width, block), 0)
    col_at = lax.broadcasted_iota(jnp.int32, (width, block), 1)
    on_diag = row_at == col_at
    holds_diag = (y_idx == z_idx).astype(F32)
    diag_here = on_diag & (y_idx == z_idx)
    off_squares = jnp.sum(jnp.where(diag_here, 0.0, covariance * covariance))
    diagonal = jnp.sum(jnp.where(on_diag, covariance, 0.0), axis=1)
    diag_mean = jnp.sum(diagonal) / width
    diag_dev = diagonal - diag_mean
    diag_m2 = jnp.sum(diag_dev * diag_dev)
    scalars = jnp.stack(
        (off_squares, holds_diag * diag_mean, holds_diag * diag_m2, holds_diag)
    )
    message = jnp.concatenate((norms, scalars))
    message = jnp.pad(message, (0, 128 - message.shape[0]))[None]

    seen = gather_small(message, SLAB).reshape(nz, nf, 128)
    count = nz * row_count
    squared = jnp.sum(seen[:, :, :count], axis=0)
    off_part = jnp.sum(seen[:, :, count])
    means, m2s, flags = seen[:, :, count + 1], seen[:, :, count + 2], seen[:, :, count + 3]
    block_mean = jnp.sum(means) / nf
    apart = flags * (means - block_mean)
    block_m2 = jnp.sum(m2s) + width * jnp.sum(apart * apart)
    second = jnp.stack(
        (jnp.sum(squared), jnp.sum(squared * squared), off_part, block_mean, block_m2)
    )
    second = jnp.pad(second, (0, 128 - second.shape[0]))[None]
    totals = gather_small(second, "y").reshape(ny, 128)
    trace_total = jnp.sum(totals[:, 0])
    fourth_total = jnp.sum(totals[:, 1])
    off_total = jnp.sum(totals[:, 2])
    mu_scale = trace_total / (total_rows * factors)
    from_mu = totals[:, 3] - mu_scale
    diag_total = jnp.sum(totals[:, 4]) + block * jnp.sum(from_mu * from_mu)
    spread = (off_total + diag_total) / factors
    norm_sq = factors * (spread + mu_scale * mu_scale)
    beta_value = (fourth_total / total_rows - norm_sq) / (factors * total_rows)
    shrinkage = beta_value / spread

    own_row = z_idx * width + lax.broadcasted_iota(jnp.int32, (width, block), 0)
    own_diag = ((own_row == col_at) & (y_idx == f_idx)).astype(F32)
    shrunk = (1.0 - shrinkage) * owned[:width] + shrinkage * mu_scale * own_diag
    return (shrunk, shrinkage, owned[width])


def solution(mesh):
    finer = Mesh(mesh.devices.reshape(8, 8, 4, 2), ("y", "z", "x", "c"))
    return jax.shard_map(
        on_device,
        mesh=finer,
        in_specs=(P(("y", "z", "x", "c"), None),),
        out_specs=(P(("y", "z"), ("x", "c")), P(), P(("x", "c"))),
        check_vma=False,
    )
```

```python
import functools

import jax
import jax.numpy as jnp
from jax import lax
from jax.experimental import pallas as pl
from jax.experimental.pallas import tpu as pltpu
from jax.sharding import Mesh
from jax.sharding import PartitionSpec as P

PLANE = ("y", "z")
SLAB = ("z", "x", "c")
EVERY = ("y", "z", "x", "c")
F32 = jnp.float32
BF16 = jnp.bfloat16
LANES = 128
NZ, NX, NC = 8, 4, 2
NF = NX * NC
SHIFT = (0, 4, 1, 7, 2, 6, 3, 5)
COLUMN = tuple(2 * (z % 4) + z // 4 for z in range(NZ))
HOLDER = tuple(COLUMN.index(block) for block in range(NZ))


def deal_rows_kernel(core_ref, x_ref, out_ref):
    block = out_ref.shape[2]

    def deal(core):
        order = [2 * x + core for x in range(NX)] + [2 * x + 1 - core for x in range(NX)]

        def one(y, carry):
            for z in range(NZ):
                for place, f in enumerate(order):
                    start = y * block + ((z + SHIFT[f]) % NZ) * LANES
                    out_ref[y * NZ + z, :, pl.ds(place * LANES, LANES)] = x_ref[
                        :, pl.ds(pl.multiple_of(start, LANES), LANES)
                    ]
            return carry

        lax.fori_loop(0, NZ, one, 0)

    @pl.when(core_ref[0] == 0)
    def _():
        deal(0)

    @pl.when(core_ref[0] == 1)
    def _():
        deal(1)


def block_kernel(place_ref, pieces_ref, mean_ref, norms_ref, packed_ref, message_ref, *, scale):
    width, block = pieces_ref.shape[1:]
    first = place_ref[0]
    lane = lax.broadcasted_iota(jnp.int32, (8, block), 1)
    sub = lax.broadcasted_iota(jnp.int32, (8, block), 0)

    def rows(step, carry):
        off, diagonal = carry
        at = pl.ds(pl.multiple_of(step * 8, 8), 8)
        tile = (pieces_ref[0, at, :] + pieces_ref[1, at, :]) + (
            pieces_ref[2, at, :] + pieces_ref[3, at, :]
        )
        tile = tile * scale
        packed_ref[at, :] = tile
        hit = lane == first + step * 8 + sub
        rest = jnp.where(hit, 0.0, tile)
        kept = jnp.where(hit, tile, 0.0)
        squares = rest * rest
        for k in range(block // LANES):
            cut = slice(k * LANES, (k + 1) * LANES)
            off = off + squares[:, cut]
            diagonal = diagonal + jnp.where(
                sub[:, :LANES] + step * 8 == lane[:, :LANES],
                jnp.sum(kept[:, cut], axis=1, keepdims=True),
                0.0,
            )
        return off, diagonal

    zero = jnp.zeros((8, LANES), F32)
    off, diagonal = lax.fori_loop(0, width // 8, rows, (zero, zero))
    packed_ref[pl.ds(width, 8), :] = jnp.broadcast_to(mean_ref[...], (8, block))

    def total(value):
        return jnp.sum(jnp.sum(value, axis=1, keepdims=True), axis=0, keepdims=True)

    flag = jnp.where(first >= 0, 1.0, 0.0)
    own = (lane[:, :LANES] % 8) == sub[:, :LANES]
    mean = total(diagonal) / width
    apart = jnp.where(own, diagonal - mean, 0.0)
    second = total(apart * apart) * flag
    norms = norms_ref[...]
    values = (
        total(norms) / NZ,
        total(norms * norms) / NZ,
        total(off),
        mean * flag,
        second,
    )
    slot = lax.broadcasted_iota(jnp.int32, (1, LANES), 1)
    message = jnp.zeros((1, LANES), F32)
    for k, value in enumerate(values):
        message = jnp.where(slot == k, value, message)
    message_ref[...] = message


def shrink_kernel(place_ref, all_ref, owned_ref, shrunk_ref, value_ref, mean_ref, *, rows, factors):
    width, block = shrunk_ref.shape
    first = place_ref[0]
    slot = lax.broadcasted_iota(jnp.int32, (1, LANES), 1)
    count = all_ref.shape[0]

    def add(step, acc):
        return acc + all_ref[pl.ds(step * 8, 8)]

    sums = lax.fori_loop(1, count // 8, add, all_ref[pl.ds(0, 8)], unroll=4)
    sums = jnp.sum(sums, axis=0)

    def pick(row, k):
        return jnp.sum(jnp.where(slot == k, row, 0.0), axis=1, keepdims=True)

    trace_total, fourth_total, off_total = (pick(sums, k) for k in range(3))
    mu_scale = trace_total / (rows * factors)
    spread_diag = jnp.zeros((1, LANES), F32)
    for y in range(NZ):
        at = (y * NZ + HOLDER[y]) * NF
        apart = all_ref[pl.ds(at, NF)] - mu_scale[None]
        spread_diag = spread_diag + jnp.sum(apart * apart, axis=0)
    diag_total = pick(sums, 4) + width * pick(spread_diag, 3)
    spread = (off_total + diag_total) / factors
    norm_sq = factors * (spread + mu_scale * mu_scale)
    beta_value = (fourth_total / rows - norm_sq) / (factors * rows)
    shrinkage = beta_value / spread
    value_ref[...] = shrinkage
    keep = 1.0 - shrinkage
    lift = shrinkage * mu_scale
    lane = lax.broadcasted_iota(jnp.int32, (8, block), 1)
    sub = lax.broadcasted_iota(jnp.int32, (8, block), 0)

    def scale_rows(step, carry):
        at = pl.ds(pl.multiple_of(step * 8, 8), 8)
        hit = lane == first + step * 8 + sub
        shrunk_ref[at, :] = keep * owned_ref[at, :] + jnp.where(hit, lift, 0.0)
        return carry

    lax.fori_loop(0, width // 8, scale_rows, 0)
    for k in range(block // LANES):
        mean_ref[pl.ds(k, 1), :] = owned_ref[pl.ds(width, 1), pl.ds(k * LANES, LANES)]


IN_VMEM = pl.BlockSpec(memory_space=pltpu.VMEM)
IN_SMEM = pl.BlockSpec(memory_space=pltpu.SMEM)


def flip(size, bit):
    return [(k, k ^ bit) for k in range(size)]


def product(left, right):
    return lax.dot_general(left, right, (((0,), (0,)), ((), ())), preferred_element_type=F32)


def on_device(scenarios):
    row_count, factors = scenarios.shape
    ny, nz = lax.axis_size("y"), lax.axis_size("z")
    plane = ny * nz
    total_rows = row_count * plane * NF
    block = factors // ny
    width = block // NF
    y_idx, z_idx, c_idx = lax.axis_index("y"), lax.axis_index("z"), lax.axis_index("c")
    f_idx = lax.axis_index(("x", "c"))
    exchange = functools.partial(lax.all_to_all, split_axis=0, concat_axis=0, tiled=True)

    dealt = pl.pallas_call(
        deal_rows_kernel,
        out_shape=jax.ShapeDtypeStruct((plane, row_count, block), BF16),
        in_specs=[IN_SMEM, IN_VMEM],
        out_specs=IN_VMEM,
        name="deal_rows",
    )(c_idx.reshape(1), scenarios)
    rows_in = exchange(dealt, PLANE)

    blocks = scenarios.reshape(row_count, 4, 2, block).transpose(2, 1, 0, 3)
    blocks = blocks.reshape(1, nz, row_count, block)
    blocks = jnp.broadcast_to(blocks, (ny, nz, row_count, block))
    cols_in = exchange(blocks.reshape(plane, row_count, block), PLANE)

    sums = jnp.sum(rows_in.astype(F32), axis=(0, 1)).reshape(8, width)
    sums = sums + jnp.roll(lax.ppermute(sums, "c", flip(NC, 1)), NX, axis=0)
    sums = sums + lax.ppermute(sums, "x", flip(NX, 1))
    sums = sums + lax.ppermute(sums, "x", flip(NX, 2))
    mean_dealt = sums / total_rows
    own = jnp.arange(8)
    to_shift = jnp.array([SHIFT[2 * x + c] for c in range(2) for x in range(NX)], jnp.int32)
    shift_here = to_shift[(c_idx * NX + own) % 8]
    slice_of = (z_idx + shift_here) % nz
    place_of = jnp.argmax(slice_of[None, :] == own[:, None], axis=1)
    mean_plain = mean_dealt[place_of]
    pairs = [(b * nz + z, z * nz + HOLDER[b]) for b in range(ny) for z in range(nz)]
    mean_c = lax.ppermute(mean_plain, PLANE, pairs).reshape(block)

    left = (rows_in.astype(F32) - mean_dealt.reshape(block)).astype(BF16)
    left = left.reshape(plane * row_count, block)
    right = (cols_in.astype(F32) - mean_c).astype(BF16)

    mine = lax.dynamic_slice_in_dim(right, y_idx * nz, nz, 0).astype(F32)
    norms = jnp.sum(mine * mine, axis=2)
    right = right.reshape(plane * row_count, block)

    half = block // 2
    swapped = lax.ppermute(product(left[:, half:], right), "c", flip(NC, 1))
    chip_sum = product(left[:, :half], right) + swapped
    pieces = exchange(chip_sum.reshape(NX, width, block), "x")

    for bit in (1, 2, 4):
        norms = norms + lax.ppermute(norms, "z", flip(NZ, bit))

    shift = jnp.array(SHIFT, jnp.int32)[f_idx]
    column = 2 * (z_idx % 4) + z_idx // 4
    slice_here = (z_idx + shift) % nz
    first = jnp.where(y_idx == column, slice_here * width, -2 * block)
    packed, message = pl.pallas_call(
        functools.partial(block_kernel, scale=1.0 / total_rows),
        out_shape=(
            jax.ShapeDtypeStruct((width + 8, block), F32),
            jax.ShapeDtypeStruct((1, LANES), F32),
        ),
        in_specs=[IN_SMEM, IN_VMEM, IN_VMEM, IN_VMEM],
        out_specs=(IN_VMEM, IN_VMEM),
        name="block_stats",
    )(first.reshape(1), pieces, mean_c.reshape(1, block), norms)

    moves = [
        (z * NF + f, ((z + SHIFT[f]) % NZ) * NF + COLUMN[z]) for z in range(NZ) for f in range(NF)
    ]
    owned = lax.ppermute(packed, SLAB, moves)
    everyone = lax.axis_size(EVERY)
    seen = exchange(jnp.broadcast_to(message[None], (everyone, 1, LANES)), EVERY)

    first_own = jnp.where(y_idx == f_idx, z_idx * width, -2 * block)
    shrunk, shrinkage, col_mean = pl.pallas_call(
        functools.partial(shrink_kernel, rows=total_rows, factors=factors),
        out_shape=(
            jax.ShapeDtypeStruct((width, block), F32),
            jax.ShapeDtypeStruct((1, 1), F32),
            jax.ShapeDtypeStruct((block // LANES, LANES), F32),
        ),
        in_specs=[IN_SMEM, IN_VMEM, IN_VMEM],
        out_specs=(IN_VMEM, IN_VMEM, IN_VMEM),
        name="shrink",
    )(first_own.reshape(1), seen, owned)
    return (shrunk, shrinkage.reshape(()), col_mean.reshape(block))


def solution(mesh):
    finer = Mesh(mesh.devices.reshape(8, NZ, NX, NC), EVERY)
    return jax.shard_map(
        on_device,
        mesh=finer,
        in_specs=(P(EVERY, None),),
        out_specs=(P(PLANE, ("x", "c")), P(), P(("x", "c"))),
        check_vma=False,
    )
```

```python
import functools

import jax
import jax.numpy as jnp
from jax import lax
from jax.experimental import pallas as pl
from jax.experimental.pallas import tpu as pltpu
from jax.sharding import Mesh
from jax.sharding import PartitionSpec as P

PLANE = ("y", "z")
LINE = ("x", "c")
SLAB = ("z", "x", "c")
EVERY = ("y", "z", "x", "c")
F32 = jnp.float32
BF16 = jnp.bfloat16
LANES = 128
NY, NZ, NX, NC = 8, 8, 4, 2
NF = NX * NC
SHIFT = (0, 4, 1, 7, 2, 6, 3, 5)
COLUMN = tuple(2 * (z % 4) + z // 4 for z in range(NZ))
HOLDER = tuple(COLUMN.index(block) for block in range(NZ))
OFF, SECOND, MEANS = 64, 65, 66
IN_VMEM = pl.BlockSpec(memory_space=pltpu.VMEM)
IN_SMEM = pl.BlockSpec(memory_space=pltpu.SMEM)


def deal_kernel(core_ref, x_ref, out_ref):
    block = out_ref.shape[3]
    half = block // 2
    core = core_ref[0]

    def take(start, size):
        return x_ref[:, pl.ds(pl.multiple_of(start, LANES), size)]

    def one(y, carry):
        for z in range(NZ):
            to = y * NZ + z
            for f in range(NF):
                at = pl.ds(f * LANES, LANES)
                out_ref[to, 0, :, at] = take(y * block + ((z + SHIFT[f]) % NZ) * LANES, LANES)
            start = COLUMN[z] * block
            out_ref[to, 1, :, pl.ds(0, half)] = take(start + core * half, half)
            out_ref[to, 1, :, pl.ds(half, half)] = take(start + (1 - core) * half, half)
        return carry

    lax.fori_loop(0, NY, one, 0)


def add_all(value):
    return jnp.sum(jnp.sum(value, axis=1, keepdims=True), axis=0, keepdims=True)


def in_lane(k, value, row):
    slot = lax.broadcasted_iota(jnp.int32, (1, LANES), 1)
    return jnp.where(slot == k, value, row)


def block_kernel(
    place_ref, pieces_ref, mean_ref, norms_ref, same_ref, other_ref, message_ref, off_ref, diag_ref, *, scale
):
    step, steps = pl.program_id(0), pl.num_programs(0)
    rows, half = pieces_ref.shape[1:]
    width = rows * steps // 2
    which = step // (steps // 2)
    base = (step % (steps // 2)) * rows
    first = place_ref[which]
    same = place_ref[2] == which
    lane = lax.broadcasted_iota(jnp.int32, (8, half), 1)
    sub = lax.broadcasted_iota(jnp.int32, (8, half), 0)

    @pl.when(step == 0)
    def _():
        off_ref[...] = jnp.zeros_like(off_ref)
        diag_ref[...] = jnp.zeros_like(diag_ref)

    off = off_ref[...]
    diagonal = diag_ref[which]
    tiles = []
    for k in range(rows // 8):
        at = pl.ds(k * 8, 8)
        tile = (pieces_ref[0, at, :] + pieces_ref[1, at, :]) + (
            pieces_ref[2, at, :] + pieces_ref[3, at, :]
        )
        tile = tile * scale
        tiles.append(tile)
        hit = lane == first + base + k * 8 + sub
        rest = jnp.where(hit, 0.0, tile)
        kept = jnp.where(hit, tile, 0.0)
        squares = rest * rest
        for j in range(half // LANES):
            cut = slice(j * LANES, (j + 1) * LANES)
            off = off + squares[:, cut]
            diagonal = diagonal + kept[:, cut]
    off_ref[...] = off
    diag_ref[which] = diagonal
    whole = jnp.concatenate(tiles, axis=0)
    to = pl.ds(pl.multiple_of(base, 8), rows)

    @pl.when(same)
    def _():
        same_ref[to, :] = whole

    @pl.when(jnp.logical_not(same))
    def _():
        other_ref[to, :] = whole

    @pl.when(step == steps - 1)
    def _():
        same_ref[pl.ds(width, 8), :] = mean_ref[...]
        own = lax.broadcasted_iota(jnp.int32, (8, LANES), 1) % 8 == lax.broadcasted_iota(
            jnp.int32, (8, LANES), 0
        )
        row = in_lane(OFF, add_all(off_ref[...]), norms_ref[...])
        flags = jnp.zeros((1, LANES), F32)
        second = jnp.zeros((1, 1), F32)
        for j in range(2):
            flag = jnp.where(place_ref[j] >= 0, 1.0, 0.0)
            mean = add_all(diag_ref[j]) / width
            apart = jnp.where(own, diag_ref[j] - mean, 0.0)
            second = second + add_all(apart * apart) * flag
            row = in_lane(MEANS + j, mean * flag, row)
            flags = in_lane(MEANS + j, flag, flags)
        row = in_lane(SECOND, second, row)
        message_ref[...] = jnp.broadcast_to(
            jnp.concatenate((row, flags), axis=0)[None], message_ref.shape
        )


def middle_kernel(seen_ref, message_ref, *, width):
    seen = seen_ref[...]
    slot = lax.broadcasted_iota(jnp.int32, (1, 1, LANES), 2)
    values, flags = seen[:, 0:1, :], seen[:, 1:2, :]
    norms = jnp.sum(values.reshape(NZ, NF, 1, LANES), axis=0)
    norms = jnp.where(slot < OFF, norms, 0.0)
    total = jnp.sum(values, axis=0)
    is_mean = (slot >= MEANS) & (slot < MEANS + 2)

    def lanes(row):
        return jnp.sum(row, axis=1, keepdims=True)

    mean = lanes(jnp.where(is_mean[0], total, 0.0)) / NF
    apart = jnp.where(is_mean, (values - mean[None]) * flags, 0.0)
    between = lanes(jnp.sum(apart * apart, axis=0))
    second = lanes(jnp.where(slot[0] == SECOND, total, 0.0)) + width * between
    row = jnp.zeros((1, LANES), F32)
    row = in_lane(0, lanes(jnp.sum(norms, axis=0)), row)
    row = in_lane(1, lanes(jnp.sum(norms * norms, axis=0)), row)
    row = in_lane(2, lanes(jnp.where(slot[0] == OFF, total, 0.0)), row)
    row = in_lane(3, mean, row)
    row = in_lane(4, second, row)
    message_ref[...] = jnp.broadcast_to(row[None], message_ref.shape)


def shrink_kernel(
    place_ref, totals_ref, same_ref, other_ref, shrunk_ref, value_ref, mean_ref, *, rows, factors
):
    width, block = shrunk_ref.shape
    half = block // 2
    first, which = place_ref[0], place_ref[1]
    slot = lax.broadcasted_iota(jnp.int32, (1, LANES), 1)
    totals = totals_ref[...]
    sums = jnp.sum(totals, axis=0)

    def pick(row, k):
        return jnp.sum(jnp.where(slot == k, row, 0.0), axis=1, keepdims=True)

    mu_scale = pick(sums, 0) / (rows * factors)
    apart = totals - mu_scale[None]
    from_mu = pick(jnp.sum(apart * apart, axis=0), 3)
    spread = (pick(sums, 2) + pick(sums, 4) + block * from_mu) / factors
    norm_sq = factors * (spread + mu_scale * mu_scale)
    beta_value = (pick(sums, 1) / rows - norm_sq) / (factors * rows)
    shrinkage = beta_value / spread
    value_ref[...] = shrinkage
    keep = 1.0 - shrinkage
    lift = shrinkage * mu_scale
    lane = lax.broadcasted_iota(jnp.int32, (8, half), 1)
    sub = lax.broadcasted_iota(jnp.int32, (8, half), 0)

    def write(source_ref, side):
        for k in range(width // 8):
            at = pl.ds(k * 8, 8)
            hit = lane + side * half == first + k * 8 + sub
            shrunk_ref[at, pl.ds(side * half, half)] = keep * source_ref[at, :] + jnp.where(
                hit, lift, 0.0
            )

    @pl.when(which == 0)
    def _():
        write(same_ref, 0)
        write(other_ref, 1)

    @pl.when(which == 1)
    def _():
        write(other_ref, 0)
        write(same_ref, 1)

    for k in range(block // LANES):
        mean_ref[pl.ds(k, 1), :] = same_ref[
            pl.ds(width + k * LANES // half, 1), pl.ds(k * LANES % half, LANES)
        ]


def flip(size):
    return [(k, k ^ 1) for k in range(size)]


def product(left, right):
    return lax.dot_general(left, right, (((0,), (0,)), ((), ())), preferred_element_type=F32)


def on_device(scenarios):
    row_count, factors = scenarios.shape
    plane = NY * NZ
    total_rows = row_count * plane * NF
    part_rows = row_count * plane
    block = factors // NY
    half, width = block // 2, block // NF
    y_idx, z_idx = lax.axis_index("y"), lax.axis_index("z")
    x_idx, c_idx = lax.axis_index("x"), lax.axis_index("c")
    f_idx = x_idx * NC + c_idx
    exchange = functools.partial(lax.all_to_all, split_axis=0, concat_axis=0, tiled=True)
    shapes = jax.ShapeDtypeStruct

    dealt = pl.pallas_call(
        deal_kernel,
        out_shape=shapes((plane, 2, row_count, block), BF16),
        in_specs=[IN_SMEM, IN_VMEM],
        out_specs=IN_VMEM,
        name="deal",
    )(c_idx.reshape(1), scenarios)
    arrived = exchange(dealt, PLANE)

    swapped = lax.ppermute(arrived, "c", flip(NC))
    sums = jnp.sum(arrived.astype(F32), axis=(0, 2))
    sums_c = jnp.where(c_idx == 0, sums[1], jnp.roll(sums[1], half))
    sums = jnp.stack((sums[0], sums_c)).reshape(2 * NF, width)
    sums = exchange(jnp.broadcast_to(sums[None], (NF, 2 * NF, width)), LINE)
    means = (jnp.sum(sums, axis=0) / total_rows).reshape(2, block)
    mean_r, mean_c = means[0], means[1]
    mean_own = jnp.where(c_idx == 0, mean_c, jnp.roll(mean_c, half))

    def centred(rows, mean):
        out = (rows.astype(F32) - mean).astype(BF16)
        return out.reshape(part_rows, out.shape[-1])

    mean_half = mean_own[:half]
    partial = product(centred(arrived[:, 0], mean_r), centred(arrived[:, 1, :, :half], mean_half))
    partial = partial + product(
        centred(swapped[:, 0], mean_r), centred(swapped[:, 1, :, half:], mean_half)
    )
    pieces = exchange(partial.reshape(NX, 2 * width, half), "x")

    mine = lax.dynamic_slice_in_dim(arrived, y_idx * NZ, NZ, 0)[:, 1]
    mine = (mine.astype(F32) - mean_own).astype(BF16).astype(F32)
    norms = jnp.sum(mine * mine, axis=2).reshape(1, NZ * row_count)
    norms = jnp.pad(norms, ((0, 0), (0, LANES - NZ * row_count)))

    shift = jnp.array(SHIFT, jnp.int32)
    column = 2 * (z_idx % 4) + z_idx // 4
    never = -2 * block
    places = []
    for j in range(2):
        piece = (z_idx + shift[x_idx * NC + j]) % NZ
        held = (y_idx == column) & (piece // 4 == c_idx)
        places.append(jnp.where(held, (piece % 4) * width, never))
    places.append(c_idx)
    steps = 4
    mean_rows = jnp.pad(mean_c.reshape(2, half), ((0, 6), (0, 0)))
    whole = lambda *dims: pl.BlockSpec(dims, lambda i: (0,) * len(dims))
    same, other, message = pl.pallas_call(
        functools.partial(block_kernel, scale=1.0 / total_rows),
        grid=(steps,),
        out_shape=(
            shapes((width + 8, half), F32),
            shapes((width, half), F32),
            shapes((NZ * NF, 2, LANES), F32),
        ),
        in_specs=[
            IN_SMEM,
            pl.BlockSpec((NX, 2 * width // steps, half), lambda i: (0, i, 0)),
            whole(8, half),
            whole(1, LANES),
        ],
        out_specs=(whole(width + 8, half), whole(width, half), whole(NZ * NF, 2, LANES)),
        scratch_shapes=[pltpu.VMEM((8, LANES), F32), pltpu.VMEM((2, 8, LANES), F32)],
        name="block_stats",
    )(jnp.stack(places), pieces, mean_rows, norms)

    seen = exchange(message, SLAB)

    def owner(z, f):
        return ((z + SHIFT[f]) % NZ) * NF + COLUMN[z]

    own_same = lax.ppermute(
        same, SLAB, [(z * NF + f, owner(z, f)) for z in range(NZ) for f in range(NF)]
    )
    own_other = lax.ppermute(
        other, SLAB, [(z * NF + f, owner(z, f ^ 1)) for z in range(NZ) for f in range(NF)]
    )
    second = pl.pallas_call(
        functools.partial(middle_kernel, width=width),
        out_shape=shapes((NY, 1, LANES), F32),
        in_specs=[IN_VMEM],
        out_specs=IN_VMEM,
        name="middle_stats",
    )(seen)
    totals = exchange(second, "y")

    first_own = jnp.where(y_idx == f_idx, z_idx * width, never)
    core_of = jnp.array([SHIFT.index(s) % 2 for s in range(NZ)], jnp.int32)
    from_z = f_idx // 2 + 4 * (f_idx % 2)
    which_own = core_of[(z_idx - from_z) % NZ]
    shrunk, shrinkage, col_mean = pl.pallas_call(
        functools.partial(shrink_kernel, rows=total_rows, factors=factors),
        out_shape=(
            shapes((width, block), F32),
            shapes((1, 1), F32),
            shapes((block // LANES, LANES), F32),
        ),
        in_specs=[IN_SMEM, IN_VMEM, IN_VMEM, IN_VMEM],
        out_specs=(IN_VMEM, IN_VMEM, IN_VMEM),
        name="shrink",
    )(jnp.stack((first_own, which_own)), totals, own_same, own_other)
    return (shrunk, shrinkage.reshape(()), col_mean.reshape(block))


def solution(mesh):
    finer = Mesh(mesh.devices.reshape(NY, NZ, NX, NC), EVERY)
    return jax.shard_map(
        on_device,
        mesh=finer,
        in_specs=(P(EVERY, None),),
        out_specs=(P(PLANE, LINE), P(), P(LINE)),
        check_vma=False,
    )
```

```python
import functools

import jax
import jax.numpy as jnp
from jax import lax
from jax.experimental import pallas as pl
from jax.experimental.pallas import tpu as pltpu
from jax.sharding import Mesh
from jax.sharding import PartitionSpec as P


PLANE = ("y", "z")
LINE = ("x", "c")
SLAB = ("z", "x", "c")
EVERY = ("y", "z", "x", "c")
F32 = jnp.float32
BF16 = jnp.bfloat16
LANES = 128
NY, NZ, NX, NC = 8, 8, 4, 2
NF = NX * NC
SHIFT = (0, 4, 1, 7, 2, 6, 3, 5)
COLUMN = tuple(2 * (z % 4) + z // 4 for z in range(NZ))
OFF, SECOND, MEANS = 64, 65, 66
IN_VMEM = pl.BlockSpec(memory_space=pltpu.VMEM)
IN_SMEM = pl.BlockSpec(memory_space=pltpu.SMEM)


def deal_kernel(core_ref, x_ref, out_ref):
    block = out_ref.shape[3]
    half = block // 2
    core = core_ref[0]

    def take(start, size):
        return x_ref[:, pl.ds(pl.multiple_of(start, LANES), size)]

    def one(y, carry):
        for z in range(NZ):
            to = y * NZ + z
            for f in range(NF):
                at = pl.ds(f * LANES, LANES)
                out_ref[to, 0, :, at] = take(y * block + ((z + SHIFT[f]) % NZ) * LANES, LANES)
            start = COLUMN[z] * block
            out_ref[to, 1, :, pl.ds(0, half)] = take(start + core * half, half)
            out_ref[to, 1, :, pl.ds(half, half)] = take(start + (1 - core) * half, half)
        return carry

    lax.fori_loop(0, NY, one, 0)


def add_all(value):
    return jnp.sum(jnp.sum(value, axis=1, keepdims=True), axis=0, keepdims=True)


def in_lane(k, value, row):
    slot = lax.broadcasted_iota(jnp.int32, (1, LANES), 1)
    return jnp.where(slot == k, value, row)


def block_kernel(
    place_ref, pieces_ref, mean_ref, norms_ref, same_ref, other_ref, message_ref, off_ref, diag_ref, *, scale
):
    step, steps = pl.program_id(0), pl.num_programs(0)
    rows, half = pieces_ref.shape[1:]
    width = rows * steps // 2
    which = step // (steps // 2)
    base = (step % (steps // 2)) * rows
    first = place_ref[which]
    same = place_ref[2] == which
    lane = lax.broadcasted_iota(jnp.int32, (8, half), 1)
    sub = lax.broadcasted_iota(jnp.int32, (8, half), 0)

    @pl.when(step == 0)
    def _():
        off_ref[...] = jnp.zeros_like(off_ref)
        diag_ref[...] = jnp.zeros_like(diag_ref)

    off = off_ref[...]
    diagonal = diag_ref[which]
    tiles = []
    for k in range(rows // 8):
        at = pl.ds(k * 8, 8)
        tile = (pieces_ref[0, at, :] + pieces_ref[1, at, :]) + (
            pieces_ref[2, at, :] + pieces_ref[3, at, :]
        )
        tile = tile * scale
        tiles.append(tile)
        hit = lane == first + base + k * 8 + sub
        rest = jnp.where(hit, 0.0, tile)
        kept = jnp.where(hit, tile, 0.0)
        squares = rest * rest
        for j in range(half // LANES):
            cut = slice(j * LANES, (j + 1) * LANES)
            off = off + squares[:, cut]
            diagonal = diagonal + kept[:, cut]
    off_ref[...] = off
    diag_ref[which] = diagonal
    whole = jnp.concatenate(tiles, axis=0)
    to = pl.ds(pl.multiple_of(base, 8), rows)

    @pl.when(same)
    def _():
        same_ref[to, :] = whole

    @pl.when(jnp.logical_not(same))
    def _():
        other_ref[to, :] = whole

    @pl.when(step == steps - 1)
    def _():
        same_ref[pl.ds(width, 8), :] = mean_ref[...]
        own = lax.broadcasted_iota(jnp.int32, (8, LANES), 1) % 8 == lax.broadcasted_iota(
            jnp.int32, (8, LANES), 0
        )
        row = in_lane(OFF, add_all(off_ref[...]), norms_ref[...])
        flags = jnp.zeros((1, LANES), F32)
        second = jnp.zeros((1, 1), F32)
        for j in range(2):
            flag = jnp.where(place_ref[j] >= 0, 1.0, 0.0)
            mean = add_all(diag_ref[j]) / width
            apart = jnp.where(own, diag_ref[j] - mean, 0.0)
            second = second + add_all(apart * apart) * flag
            row = in_lane(MEANS + j, mean * flag, row)
            flags = in_lane(MEANS + j, flag, flags)
        row = in_lane(SECOND, second, row)
        message_ref[...] = jnp.broadcast_to(
            jnp.concatenate((row, flags), axis=0)[None], message_ref.shape
        )


def middle_kernel(seen_ref, message_ref, *, width):
    seen = seen_ref[...]
    slot = lax.broadcasted_iota(jnp.int32, (1, 1, LANES), 2)
    values, flags = seen[:, 0:1, :], seen[:, 1:2, :]
    norms = jnp.sum(values.reshape(NZ, NF, 1, LANES), axis=0)
    norms = jnp.where(slot < OFF, norms, 0.0)
    total = jnp.sum(values, axis=0)
    is_mean = (slot >= MEANS) & (slot < MEANS + 2)

    def lanes(row):
        return jnp.sum(row, axis=1, keepdims=True)

    mean = lanes(jnp.where(is_mean[0], total, 0.0)) / NF
    apart = jnp.where(is_mean, (values - mean[None]) * flags, 0.0)
    between = lanes(jnp.sum(apart * apart, axis=0))
    second = lanes(jnp.where(slot[0] == SECOND, total, 0.0)) + width * between
    row = jnp.zeros((1, LANES), F32)
    row = in_lane(0, lanes(jnp.sum(norms, axis=0)), row)
    row = in_lane(1, lanes(jnp.sum(norms * norms, axis=0)), row)
    row = in_lane(2, lanes(jnp.where(slot[0] == OFF, total, 0.0)), row)
    row = in_lane(3, mean, row)
    row = in_lane(4, second, row)
    message_ref[...] = jnp.broadcast_to(row[None], message_ref.shape)


def shrink_kernel(
    place_ref, totals_ref, same_ref, other_ref, shrunk_ref, value_ref, mean_ref, *, rows, factors
):
    width, block = shrunk_ref.shape
    half = block // 2
    first, which = place_ref[0], place_ref[1]
    slot = lax.broadcasted_iota(jnp.int32, (1, LANES), 1)
    totals = totals_ref[...]
    sums = jnp.sum(totals, axis=0)

    def pick(row, k):
        return jnp.sum(jnp.where(slot == k, row, 0.0), axis=1, keepdims=True)

    mu_scale = pick(sums, 0) / (rows * factors)
    apart = totals - mu_scale[None]
    from_mu = pick(jnp.sum(apart * apart, axis=0), 3)
    spread = (pick(sums, 2) + pick(sums, 4) + block * from_mu) / factors
    norm_sq = factors * (spread + mu_scale * mu_scale)
    beta_value = (pick(sums, 1) / rows - norm_sq) / (factors * rows)
    shrinkage = beta_value / spread
    value_ref[...] = shrinkage
    keep = 1.0 - shrinkage
    lift = shrinkage * mu_scale
    lane = lax.broadcasted_iota(jnp.int32, (8, half), 1)
    sub = lax.broadcasted_iota(jnp.int32, (8, half), 0)

    def write(source_ref, side):
        for k in range(width // 8):
            at = pl.ds(k * 8, 8)
            hit = lane + side * half == first + k * 8 + sub
            shrunk_ref[at, pl.ds(side * half, half)] = keep * source_ref[at, :] + jnp.where(
                hit, lift, 0.0
            )

    @pl.when(which == 0)
    def _():
        write(same_ref, 0)
        write(other_ref, 1)

    @pl.when(which == 1)
    def _():
        write(other_ref, 0)
        write(same_ref, 1)

    for k in range(block // LANES):
        mean_ref[pl.ds(k, 1), :] = same_ref[
            pl.ds(width + k * LANES // half, 1), pl.ds(k * LANES % half, LANES)
        ]


def flip(size):
    return [(k, k ^ 1) for k in range(size)]


def product(left, right):
    return lax.dot_general(left, right, (((0,), (0,)), ((), ())), preferred_element_type=F32)


def shrinkage_step(scenarios):
    row_count, factors = scenarios.shape
    plane = NY * NZ
    total_rows = row_count * plane * NF
    part_rows = row_count * plane
    block = factors // NY
    half, width = block // 2, block // NF
    y_idx, z_idx = lax.axis_index("y"), lax.axis_index("z")
    x_idx, c_idx = lax.axis_index("x"), lax.axis_index("c")
    f_idx = x_idx * NC + c_idx
    exchange = functools.partial(lax.all_to_all, split_axis=0, concat_axis=0, tiled=True)
    shapes = jax.ShapeDtypeStruct

    dealt = pl.pallas_call(
        deal_kernel,
        out_shape=shapes((plane, 2, row_count, block), BF16),
        in_specs=[IN_SMEM, IN_VMEM],
        out_specs=IN_VMEM,
        name="deal",
    )(c_idx.reshape(1), scenarios)
    arrived = exchange(dealt, PLANE)

    swapped = lax.ppermute(arrived, "c", flip(NC))
    sums = jnp.sum(arrived.astype(F32), axis=(0, 2))
    sums_c = jnp.where(c_idx == 0, sums[1], jnp.roll(sums[1], half))
    sums = jnp.stack((sums[0], sums_c)).reshape(2 * NF, width)
    sums = exchange(jnp.broadcast_to(sums[None], (NF, 2 * NF, width)), LINE)
    means = (jnp.sum(sums, axis=0) / total_rows).reshape(2, block)
    mean_r, mean_c = means[0], means[1]
    mean_own = jnp.where(c_idx == 0, mean_c, jnp.roll(mean_c, half))

    def centred(rows, mean):
        out = (rows.astype(F32) - mean).astype(BF16)
        return out.reshape(part_rows, out.shape[-1])

    mean_half = mean_own[:half]
    partial = product(centred(arrived[:, 0], mean_r), centred(arrived[:, 1, :, :half], mean_half))
    partial = partial + product(
        centred(swapped[:, 0], mean_r), centred(swapped[:, 1, :, half:], mean_half)
    )
    pieces = exchange(partial.reshape(NX, 2 * width, half), "x")

    mine = lax.dynamic_slice_in_dim(arrived, y_idx * NZ, NZ, 0)[:, 1]
    mine = (mine.astype(F32) - mean_own).astype(BF16).astype(F32)
    norms = jnp.sum(mine * mine, axis=2).reshape(1, NZ * row_count)
    norms = jnp.pad(norms, ((0, 0), (0, LANES - NZ * row_count)))

    shift = jnp.array(SHIFT, jnp.int32)
    column = 2 * (z_idx % 4) + z_idx // 4
    never = -2 * block
    places = []
    for j in range(2):
        piece = (z_idx + shift[x_idx * NC + j]) % NZ
        held = (y_idx == column) & (piece // 4 == c_idx)
        places.append(jnp.where(held, (piece % 4) * width, never))
    places.append(c_idx)
    steps = 4
    mean_rows = jnp.pad(mean_c.reshape(2, half), ((0, 6), (0, 0)))
    whole = lambda *dims: pl.BlockSpec(dims, lambda i: (0,) * len(dims))
    same, other, message = pl.pallas_call(
        functools.partial(block_kernel, scale=1.0 / total_rows),
        grid=(steps,),
        out_shape=(
            shapes((width + 8, half), F32),
            shapes((width, half), F32),
            shapes((NZ * NF, 2, LANES), F32),
        ),
        in_specs=[
            IN_SMEM,
            pl.BlockSpec((NX, 2 * width // steps, half), lambda i: (0, i, 0)),
            whole(8, half),
            whole(1, LANES),
        ],
        out_specs=(whole(width + 8, half), whole(width, half), whole(NZ * NF, 2, LANES)),
        scratch_shapes=[pltpu.VMEM((8, LANES), F32), pltpu.VMEM((2, 8, LANES), F32)],
        name="block_stats",
    )(jnp.stack(places), pieces, mean_rows, norms)

    seen = exchange(message, SLAB)

    def owner(z, f):
        return ((z + SHIFT[f]) % NZ) * NF + COLUMN[z]

    own_same = lax.ppermute(
        same, SLAB, [(z * NF + f, owner(z, f)) for z in range(NZ) for f in range(NF)]
    )
    own_other = lax.ppermute(
        other, SLAB, [(z * NF + f, owner(z, f ^ 1)) for z in range(NZ) for f in range(NF)]
    )
    second = pl.pallas_call(
        functools.partial(middle_kernel, width=width),
        out_shape=shapes((NY, 1, LANES), F32),
        in_specs=[IN_VMEM],
        out_specs=IN_VMEM,
        name="middle_stats",
    )(seen)
    totals = exchange(second, "y")

    first_own = jnp.where(y_idx == f_idx, z_idx * width, never)
    core_of = jnp.array([SHIFT.index(s) % 2 for s in range(NZ)], jnp.int32)
    from_z = f_idx // 2 + 4 * (f_idx % 2)
    which_own = core_of[(z_idx - from_z) % NZ]
    shrunk, shrinkage, col_mean = pl.pallas_call(
        functools.partial(shrink_kernel, rows=total_rows, factors=factors),
        out_shape=(
            shapes((width, block), F32),
            shapes((1, 1), F32),
            shapes((block // LANES, LANES), F32),
        ),
        in_specs=[IN_SMEM, IN_VMEM, IN_VMEM, IN_VMEM],
        out_specs=(IN_VMEM, IN_VMEM, IN_VMEM),
        name="shrink",
    )(jnp.stack((first_own, which_own)), totals, own_same, own_other)
    return (shrunk, shrinkage.reshape(()), col_mean.reshape(block))


def solution(mesh):
    finer = Mesh(mesh.devices.reshape(NY, NZ, NX, NC), EVERY)
    return jax.shard_map(
        shrinkage_step,
        mesh=finer,
        in_specs=(P(EVERY, None),),
        out_specs=(P(PLANE, LINE), P(), P(LINE)),
        check_vma=False,
    )
```

```python
import functools

import jax
import jax.numpy as jnp
from jax import lax
from jax.experimental import pallas as pl
from jax.experimental.pallas import tpu as pltpu
from jax.sharding import Mesh
from jax.sharding import PartitionSpec as P


PLANE = ("y", "z")
LINE = ("x", "c")
SLAB = ("z", "x", "c")
EVERY = ("y", "z", "x", "c")
F32 = jnp.float32
BF16 = jnp.bfloat16
LANES = 128
NY, NZ, NX, NC = 8, 8, 4, 2
NF = NX * NC
SHIFT = (0, 4, 1, 7, 2, 6, 3, 5)
COLUMN = tuple(2 * (z % 4) + z // 4 for z in range(NZ))
OFF, SECOND, MEANS = 64, 65, 66
HEADER = 8
F16 = jnp.float16
IN_VMEM = pl.BlockSpec(memory_space=pltpu.VMEM)
IN_SMEM = pl.BlockSpec(memory_space=pltpu.SMEM)


def deal_kernel(core_ref, x_ref, out_ref):
    block = out_ref.shape[3]
    half = block // 2
    core = core_ref[0]

    def take(start, size):
        return x_ref[:, pl.ds(pl.multiple_of(start, LANES), size)]

    def one(y, carry):
        for z in range(NZ):
            to = y * NZ + z
            for f in range(NF):
                at = pl.ds(f * LANES, LANES)
                out_ref[to, 0, :, at] = take(y * block + ((z + SHIFT[f]) % NZ) * LANES, LANES)
            start = COLUMN[z] * block
            out_ref[to, 1, :, pl.ds(0, half)] = take(start + core * half, half)
            out_ref[to, 1, :, pl.ds(half, half)] = take(start + (1 - core) * half, half)
        return carry

    lax.fori_loop(0, NY, one, 0)


def add_all(value):
    return jnp.sum(jnp.sum(value, axis=1, keepdims=True), axis=0, keepdims=True)


def half_power(top):
    return jnp.clip(jnp.floor(jnp.log2(jnp.maximum(top, 1e-30))), -90.0, 90.0) - 13.0


def in_lane(k, value, row):
    slot = lax.broadcasted_iota(jnp.int32, (1, LANES), 1)
    return jnp.where(slot == k, value, row)


def block_kernel(place_ref, sum_ref, norms_ref, same_ref, other_ref, message_ref):
    width, half = same_ref.shape[0] - HEADER, same_ref.shape[1]
    lane = lax.broadcasted_iota(jnp.int32, (8, half), 1)
    sub = lax.broadcasted_iota(jnp.int32, (8, half), 0)
    cuts = [slice(j * LANES, (j + 1) * LANES) for j in range(half // LANES)]
    zero = jnp.zeros((8, LANES), F32)
    off, top, diagonals = zero, zero, []
    for j in range(2):
        diagonal = zero
        for k in range(width // 8):
            tile = sum_ref[pl.ds(j * width + k * 8, 8), :]
            hit = lane == place_ref[j] + k * 8 + sub
            rest = jnp.where(hit, 0.0, tile)
            kept = jnp.where(hit, tile, 0.0)
            squares, size = rest * rest, jnp.abs(tile)
            for cut in cuts:
                off = off + squares[:, cut]
                diagonal = diagonal + kept[:, cut]
                top = jnp.maximum(top, size[:, cut])
        diagonals.append(diagonal)
    top = jnp.max(jnp.max(top, axis=1, keepdims=True), axis=0, keepdims=True)
    power = half_power(top)
    factor = jnp.exp2(-power)

    def write(out_ref, j):
        for k in range(width // 8):
            out_ref[pl.ds(k * 8, 8), :] = sum_ref[pl.ds(j * width + k * 8, 8), :] * factor
        out_ref[pl.ds(width, HEADER), :] = jnp.broadcast_to(power, (HEADER, half))

    @pl.when(place_ref[2] == 0)
    def _():
        write(same_ref, 0)
        write(other_ref, 1)

    @pl.when(place_ref[2] == 1)
    def _():
        write(same_ref, 1)
        write(other_ref, 0)

    own = lane[:, :LANES] % 8 == sub[:, :LANES]
    row = in_lane(OFF, add_all(off), norms_ref[...])
    flags = jnp.zeros((1, LANES), F32)
    second = jnp.zeros((1, 1), F32)
    for j in range(2):
        flag = jnp.where(place_ref[j] >= 0, 1.0, 0.0)
        mean = add_all(diagonals[j]) / width
        apart = jnp.where(own, diagonals[j] - mean, 0.0)
        second = second + add_all(apart * apart) * flag
        row = in_lane(MEANS + j, mean * flag, row)
        flags = in_lane(MEANS + j, flag, flags)
    row = in_lane(SECOND, second, row)
    message_ref[...] = jnp.broadcast_to(
        jnp.concatenate((row, flags), axis=0)[None], message_ref.shape
    )


def middle_kernel(seen_ref, message_ref, *, width):
    seen = seen_ref[...]
    slot = lax.broadcasted_iota(jnp.int32, (1, 1, LANES), 2)
    values, flags = seen[:, 0:1, :], seen[:, 1:2, :]
    norms = jnp.sum(values.reshape(NZ, NF, 1, LANES), axis=0)
    norms = jnp.where(slot < OFF, norms, 0.0)
    total = jnp.sum(values, axis=0)
    is_mean = (slot >= MEANS) & (slot < MEANS + 2)

    def lanes(row):
        return jnp.sum(row, axis=1, keepdims=True)

    mean = lanes(jnp.where(is_mean[0], total, 0.0)) / NF
    apart = jnp.where(is_mean, (values - mean[None]) * flags, 0.0)
    between = lanes(jnp.sum(apart * apart, axis=0))
    second = lanes(jnp.where(slot[0] == SECOND, total, 0.0)) + width * between
    row = jnp.zeros((1, LANES), F32)
    row = in_lane(0, lanes(jnp.sum(norms, axis=0)), row)
    row = in_lane(1, lanes(jnp.sum(norms * norms, axis=0)), row)
    row = in_lane(2, lanes(jnp.where(slot[0] == OFF, total, 0.0)), row)
    row = in_lane(3, mean, row)
    row = in_lane(4, second, row)
    message_ref[...] = jnp.broadcast_to(row[None], message_ref.shape)


def shrink_kernel(
    place_ref, totals_ref, same_ref, other_ref, shrunk_ref, value_ref, *, rows, factors
):
    width, block = shrunk_ref.shape
    half = block // 2
    first, which = place_ref[0], place_ref[1]
    slot = lax.broadcasted_iota(jnp.int32, (1, LANES), 1)
    totals = totals_ref[...]
    sums = jnp.sum(totals, axis=0)

    def pick(row, k):
        return jnp.sum(jnp.where(slot == k, row, 0.0), axis=1, keepdims=True)

    mu_scale = pick(sums, 0) / (rows * factors)
    apart = totals - mu_scale[None]
    from_mu = pick(jnp.sum(apart * apart, axis=0), 3)
    spread = (pick(sums, 2) + pick(sums, 4) + block * from_mu) / factors
    norm_sq = factors * (spread + mu_scale * mu_scale)
    beta_value = (pick(sums, 1) / rows - norm_sq) / (factors * rows)
    shrinkage = beta_value / spread
    value_ref[...] = shrinkage
    keep = 1.0 - shrinkage
    lift = shrinkage * mu_scale
    lane = lax.broadcasted_iota(jnp.int32, (8, half), 1)
    sub = lax.broadcasted_iota(jnp.int32, (8, half), 0)

    def write(source_ref, side):
        for k in range(width // 8):
            at = pl.ds(k * 8, 8)
            hit = lane + side * half == first + k * 8 + sub
            shrunk_ref[at, pl.ds(side * half, half)] = keep * source_ref[at, :] + jnp.where(
                hit, lift, 0.0
            )

    @pl.when(which == 0)
    def _():
        write(same_ref, 0)
        write(other_ref, 1)

    @pl.when(which == 1)
    def _():
        write(other_ref, 0)
        write(same_ref, 1)


def flip(size):
    return [(k, k ^ 1) for k in range(size)]


def product(left, right):
    return lax.dot_general(left, right, (((0,), (0,)), ((), ())), preferred_element_type=F32)


def shrinkage_step(scenarios):
    row_count, factors = scenarios.shape
    plane = NY * NZ
    total_rows = row_count * plane * NF
    part_rows = row_count * plane
    block = factors // NY
    half, width = block // 2, block // NF
    y_idx, z_idx = lax.axis_index("y"), lax.axis_index("z")
    x_idx, c_idx = lax.axis_index("x"), lax.axis_index("c")
    f_idx = x_idx * NC + c_idx
    exchange = functools.partial(lax.all_to_all, split_axis=0, concat_axis=0, tiled=True)
    shapes = jax.ShapeDtypeStruct

    dealt = pl.pallas_call(
        deal_kernel,
        out_shape=shapes((plane, 2, row_count, block), BF16),
        in_specs=[IN_SMEM, IN_VMEM],
        out_specs=IN_VMEM,
        name="deal",
    )(c_idx.reshape(1), scenarios)
    arrived = exchange(dealt, PLANE)

    swapped = lax.ppermute(arrived, "c", flip(NC))
    sums = jnp.sum(arrived.astype(F32), axis=(0, 2))
    sums_c = jnp.where(c_idx == 0, sums[1], jnp.roll(sums[1], half))
    sums = jnp.stack((sums[0], sums_c)).reshape(2 * NF, width)
    sums = exchange(jnp.broadcast_to(sums[None], (NF, 2 * NF, width)), LINE)
    means = (jnp.sum(sums, axis=0) / total_rows).reshape(2, block)
    mean_r, mean_c = means[0], means[1]
    mean_own = jnp.where(c_idx == 0, mean_c, jnp.roll(mean_c, half))

    def centred(rows, mean):
        out = (rows.astype(F32) - mean).astype(BF16)
        return out.reshape(part_rows, out.shape[-1])

    mean_half = mean_own[:half]
    partial = product(centred(arrived[:, 0], mean_r), centred(arrived[:, 1, :, :half], mean_half))
    partial = partial + product(
        centred(swapped[:, 0], mean_r), centred(swapped[:, 1, :, half:], mean_half)
    )
    partial = partial * (1.0 / total_rows)
    power = half_power(jnp.max(jnp.abs(partial)))
    parcel = jnp.pad(partial.reshape(NX, 2 * width, half), ((0, 0), (0, HEADER), (0, 0)))
    at_row = lax.broadcasted_iota(jnp.int32, parcel.shape, 1)
    parcel = jnp.where(at_row < 2 * width, parcel * jnp.exp2(-power), power).astype(F16)
    pieces = exchange(parcel, "x")
    powers = jnp.exp2(pieces[:, 2 * width, 0].astype(F32))
    summed = jnp.sum(pieces[:, : 2 * width].astype(F32) * powers[:, None, None], axis=0)

    mine = lax.dynamic_slice_in_dim(arrived, y_idx * NZ, NZ, 0)[:, 1]
    mine = (mine.astype(F32) - mean_own).astype(BF16).astype(F32)
    norms = jnp.sum(mine * mine, axis=2).reshape(1, NZ * row_count)
    norms = jnp.pad(norms, ((0, 0), (0, LANES - NZ * row_count)))

    shift = jnp.array(SHIFT, jnp.int32)
    column = 2 * (z_idx % 4) + z_idx // 4
    never = -2 * block
    places = []
    for j in range(2):
        piece = (z_idx + shift[x_idx * NC + j]) % NZ
        held = (y_idx == column) & (piece // 4 == c_idx)
        places.append(jnp.where(held, (piece % 4) * width, never))
    places.append(c_idx)
    same, other, message = pl.pallas_call(
        block_kernel,
        out_shape=(
            shapes((width + HEADER, half), F32),
            shapes((width + HEADER, half), F32),
            shapes((NZ * NF, 2, LANES), F32),
        ),
        in_specs=[IN_SMEM, IN_VMEM, IN_VMEM],
        out_specs=(IN_VMEM, IN_VMEM, IN_VMEM),
        name="block_stats",
    )(jnp.stack(places), summed, norms)

    seen = exchange(message, SLAB)

    def owner(z, f):
        return ((z + SHIFT[f]) % NZ) * NF + COLUMN[z]

    to_same = [(z * NF + f, owner(z, f)) for z in range(NZ) for f in range(NF)]
    to_other = [(z * NF + f, owner(z, f ^ 1)) for z in range(NZ) for f in range(NF)]

    def unpack(block):
        return block[:width].astype(F32) * jnp.exp2(block[width, 0].astype(F32))

    own_same = unpack(lax.ppermute(same.astype(F16), SLAB, to_same))
    own_other = unpack(lax.ppermute(other.astype(F16), SLAB, to_other))
    col_mean = lax.ppermute(mean_c.reshape(NF, width), SLAB, to_same).reshape(block)
    second = pl.pallas_call(
        functools.partial(middle_kernel, width=width),
        out_shape=shapes((NY, 1, LANES), F32),
        in_specs=[IN_VMEM],
        out_specs=IN_VMEM,
        name="middle_stats",
    )(seen)
    totals = exchange(second, "y")

    first_own = jnp.where(y_idx == f_idx, z_idx * width, never)
    core_of = jnp.array([SHIFT.index(s) % 2 for s in range(NZ)], jnp.int32)
    from_z = f_idx // 2 + 4 * (f_idx % 2)
    which_own = core_of[(z_idx - from_z) % NZ]
    shrunk, shrinkage = pl.pallas_call(
        functools.partial(shrink_kernel, rows=total_rows, factors=factors),
        out_shape=(
            shapes((width, block), F32),
            shapes((1, 1), F32),
        ),
        in_specs=[IN_SMEM, IN_VMEM, IN_VMEM, IN_VMEM],
        out_specs=(IN_VMEM, IN_VMEM),
        name="shrink",
    )(jnp.stack((first_own, which_own)), totals, own_same, own_other)
    return (shrunk, shrinkage.reshape(()), col_mean)


def solution(mesh):
    finer = Mesh(mesh.devices.reshape(NY, NZ, NX, NC), EVERY)
    return jax.shard_map(
        shrinkage_step,
        mesh=finer,
        in_specs=(P(EVERY, None),),
        out_specs=(P(PLANE, LINE), P(), P(LINE)),
        check_vma=False,
    )
```

```python
import functools

import jax
import jax.numpy as jnp
from jax import lax
from jax.experimental import pallas as pl
from jax.experimental.pallas import tpu as pltpu
from jax.sharding import Mesh
from jax.sharding import PartitionSpec as P


PLANE = ("y", "z")
LINE = ("x", "c")
SLAB = ("z", "x", "c")
EVERY = ("y", "z", "x", "c")
F32 = jnp.float32
BF16 = jnp.bfloat16
LANES = 128
NY, NZ, NX, NC = 8, 8, 4, 2
NF = NX * NC
SHIFT = (0, 4, 1, 7, 2, 6, 3, 5)
COLUMN = tuple(2 * (z % 4) + z // 4 for z in range(NZ))
OFF, SECOND, MEANS = 64, 65, 66
F16 = jnp.float16
IN_VMEM = pl.BlockSpec(memory_space=pltpu.VMEM)
IN_SMEM = pl.BlockSpec(memory_space=pltpu.SMEM)


def deal_kernel(core_ref, x_ref, out_ref):
    block = out_ref.shape[3]

    def take(start, size):
        return x_ref[:, pl.ds(pl.multiple_of(start, LANES), size)]

    def deal(core):
        order = [2 * x + core for x in range(NX)] + [2 * x + 1 - core for x in range(NX)]

        def one(y, carry):
            for z in range(NZ):
                to = y * NZ + z
                for place, f in enumerate(order):
                    start = y * block + ((z + SHIFT[f]) % NZ) * LANES
                    out_ref[to, 0, :, pl.ds(place * LANES, LANES)] = take(start, LANES)
                out_ref[to, 1] = take(COLUMN[z] * block, block)
            return carry

        lax.fori_loop(0, NY, one, 0)

    for core in range(NC):
        pl.when(core_ref[0] == core)(functools.partial(deal, core))


def add_all(value):
    return jnp.sum(jnp.sum(value, axis=1, keepdims=True), axis=0, keepdims=True)


def half_power(top):
    return jnp.clip(jnp.floor(jnp.log2(jnp.maximum(top, 1e-30))), -90.0, 90.0) - 13.0


def in_lane(k, value, row):
    slot = lax.broadcasted_iota(jnp.int32, (1, LANES), 1)
    return jnp.where(slot == k, value, row)


def block_kernel(place_ref, sum_ref, norms_ref, factor_ref, message_ref):
    width, block = sum_ref.shape
    lane = lax.broadcasted_iota(jnp.int32, (8, block), 1)
    sub = lax.broadcasted_iota(jnp.int32, (8, block), 0)
    first, factor = place_ref[0], factor_ref[0]
    zero = jnp.zeros((8, LANES), F32)
    off, diagonal = zero, zero
    for k in range(width // 8):
        tile = sum_ref[pl.ds(k * 8, 8), :] * factor
        hit = lane == first + k * 8 + sub
        rest = jnp.where(hit, 0.0, tile)
        kept = jnp.where(hit, tile, 0.0)
        squares = rest * rest
        for j in range(block // LANES):
            cut = slice(j * LANES, (j + 1) * LANES)
            off = off + squares[:, cut]
            diagonal = diagonal + kept[:, cut]
    own = lane[:, :LANES] % 8 == sub[:, :LANES]
    flag = jnp.where(first >= 0, 1.0, 0.0)
    mean = add_all(diagonal) / width
    apart = jnp.where(own, diagonal - mean, 0.0)
    row = in_lane(OFF, add_all(off), norms_ref[...])
    row = in_lane(SECOND, add_all(apart * apart) * flag, row)
    row = in_lane(MEANS, mean * flag, row)
    flags = in_lane(MEANS, flag, jnp.zeros((1, LANES), F32))
    message_ref[...] = jnp.broadcast_to(
        jnp.concatenate((row, flags), axis=0)[None], message_ref.shape
    )


def middle_kernel(seen_ref, message_ref, *, width):
    seen = seen_ref[...]
    slot = lax.broadcasted_iota(jnp.int32, (1, 1, LANES), 2)
    values, flags = seen[:, 0:1, :], seen[:, 1:2, :]
    norms = jnp.sum(values.reshape(NZ, NF, 1, LANES), axis=0)
    norms = jnp.where(slot < OFF, norms, 0.0)
    total = jnp.sum(values, axis=0)
    is_mean = slot == MEANS

    def lanes(row):
        return jnp.sum(row, axis=1, keepdims=True)

    mean = lanes(jnp.where(is_mean[0], total, 0.0)) / NF
    apart = jnp.where(is_mean, (values - mean[None]) * flags, 0.0)
    between = lanes(jnp.sum(apart * apart, axis=0))
    second = lanes(jnp.where(slot[0] == SECOND, total, 0.0)) + width * between
    row = jnp.zeros((1, LANES), F32)
    row = in_lane(0, lanes(jnp.sum(norms, axis=0)), row)
    row = in_lane(1, lanes(jnp.sum(norms * norms, axis=0)), row)
    row = in_lane(2, lanes(jnp.where(slot[0] == OFF, total, 0.0)), row)
    row = in_lane(3, mean, row)
    row = in_lane(4, second, row)
    message_ref[...] = jnp.broadcast_to(row[None], message_ref.shape)


def shrink_kernel(place_ref, factor_ref, totals_ref, owned_ref, shrunk_ref, value_ref, *, rows, factors):
    width, block = shrunk_ref.shape
    first = place_ref[0]
    slot = lax.broadcasted_iota(jnp.int32, (1, LANES), 1)
    totals = totals_ref[...]
    sums = jnp.sum(totals, axis=0)

    def pick(row, k):
        return jnp.sum(jnp.where(slot == k, row, 0.0), axis=1, keepdims=True)

    mu_scale = pick(sums, 0) / (rows * factors)
    apart = totals - mu_scale[None]
    from_mu = pick(jnp.sum(apart * apart, axis=0), 3)
    spread = (pick(sums, 2) + pick(sums, 4) + block * from_mu) / factors
    norm_sq = factors * (spread + mu_scale * mu_scale)
    beta_value = (pick(sums, 1) / rows - norm_sq) / (factors * rows)
    shrinkage = beta_value / spread
    value_ref[...] = shrinkage
    keep = (1.0 - shrinkage) * factor_ref[0]
    lift = shrinkage * mu_scale
    lane = lax.broadcasted_iota(jnp.int32, (8, block), 1)
    sub = lax.broadcasted_iota(jnp.int32, (8, block), 0)
    for k in range(width // 8):
        at = pl.ds(k * 8, 8)
        hit = lane == first + k * 8 + sub
        shrunk_ref[at, :] = keep * owned_ref[at, :] + jnp.where(hit, lift, 0.0)


def flip(size):
    return [(k, k ^ 1) for k in range(size)]


def product(left, right):
    return lax.dot_general(left, right, (((0,), (0,)), ((), ())), preferred_element_type=F32)


def shrinkage_step(scenarios):
    row_count, factors = scenarios.shape
    plane = NY * NZ
    total_rows = row_count * plane * NF
    part_rows = row_count * plane
    block = factors // NY
    half, width = block // 2, block // NF
    y_idx, z_idx = lax.axis_index("y"), lax.axis_index("z")
    x_idx, c_idx = lax.axis_index("x"), lax.axis_index("c")
    f_idx = x_idx * NC + c_idx
    exchange = functools.partial(lax.all_to_all, split_axis=0, concat_axis=0, tiled=True)
    shapes = jax.ShapeDtypeStruct

    dealt = pl.pallas_call(
        deal_kernel,
        out_shape=shapes((plane, 2, row_count, block), BF16),
        in_specs=[IN_SMEM, IN_VMEM],
        out_specs=IN_VMEM,
        name="deal",
    )(c_idx.reshape(1), scenarios)
    arrived = exchange(dealt, PLANE)

    swapped = lax.ppermute(arrived, "c", flip(NC))
    values = arrived.astype(F32)
    sums = jnp.sum(values, axis=(0, 2))
    wide = jnp.max(jnp.abs(values - values[:1, :, :1]), axis=(0, 2))
    sums_r = jnp.where(c_idx == 0, sums[0], jnp.roll(sums[0], half))
    told = jnp.concatenate((sums_r.reshape(NF, width), sums[1].reshape(NF, width)))
    told = jnp.concatenate((told, jnp.broadcast_to(jnp.max(wide), (8, width))))
    told = exchange(jnp.broadcast_to(told[None], (NF, *told.shape)), LINE)
    part = told[:, : 2 * NF] / part_rows
    means = jnp.sum(told[:, : 2 * NF], axis=0) / total_rows
    reach = 2.0 * jnp.max(told[:, 2 * NF]) + jnp.max(jnp.abs(part - means))
    power = half_power(reach * reach)
    mean_c = means[NF:].reshape(block)
    mean_r = means[:NF].reshape(2, half)
    mean_half = jnp.where(c_idx == 0, mean_r[0], mean_r[1])

    def centred(rows, mean):
        out = (rows.astype(F32) - mean).astype(BF16)
        return out.reshape(part_rows, out.shape[-1])

    partial = product(centred(arrived[:, 0, :, :half], mean_half), centred(arrived[:, 1], mean_c))
    partial = partial + product(
        centred(swapped[:, 0, :, half:], mean_half), centred(swapped[:, 1], mean_c)
    )
    parcel = (partial * (jnp.exp2(-power) / total_rows)).astype(F16)
    pieces = exchange(parcel.reshape(NX, width, block), "x")
    summed = jnp.sum(pieces.astype(F32), axis=0)

    mine = lax.dynamic_slice_in_dim(arrived, y_idx * NZ, NZ, 0)[:, 1]
    mine = (mine.astype(F32) - mean_c).astype(BF16).astype(F32)
    norms = jnp.sum(mine * mine, axis=2).reshape(1, NZ * row_count)
    norms = jnp.pad(norms, ((0, 0), (0, LANES - NZ * row_count)))

    shift = jnp.array(SHIFT, jnp.int32)[f_idx]
    column = 2 * (z_idx % 4) + z_idx // 4
    never = -2 * block
    first = jnp.where(y_idx == column, (z_idx + shift) % NZ * width, never)
    message = pl.pallas_call(
        block_kernel,
        out_shape=shapes((NZ * NF, 2, LANES), F32),
        in_specs=[IN_SMEM, IN_VMEM, IN_VMEM, IN_SMEM],
        out_specs=IN_VMEM,
        name="block_stats",
    )(first.reshape(1), summed, norms, jnp.exp2(power).reshape(1))

    seen = exchange(message, SLAB)

    def owner(z, f):
        return ((z + SHIFT[f]) % NZ) * NF + COLUMN[z]

    moves = [(z * NF + f, owner(z, f)) for z in range(NZ) for f in range(NF)]
    owned = lax.ppermute(summed.astype(F16), SLAB, moves).astype(F32)
    carried = jnp.concatenate(
        (mean_c.reshape(NF, width), jnp.broadcast_to(power, (8, width)))
    )
    carried = lax.ppermute(carried, SLAB, moves)
    second = pl.pallas_call(
        functools.partial(middle_kernel, width=width),
        out_shape=shapes((NY, 1, LANES), F32),
        in_specs=[IN_VMEM],
        out_specs=IN_VMEM,
        name="middle_stats",
    )(seen)
    totals = exchange(second, "y")

    first_own = jnp.where(y_idx == f_idx, z_idx * width, never)
    shrunk, shrinkage = pl.pallas_call(
        functools.partial(shrink_kernel, rows=total_rows, factors=factors),
        out_shape=(shapes((width, block), F32), shapes((1, 1), F32)),
        in_specs=[IN_SMEM, IN_SMEM, IN_VMEM, IN_VMEM],
        out_specs=(IN_VMEM, IN_VMEM),
        name="shrink",
    )(first_own.reshape(1), jnp.exp2(carried[NF, :1]), totals, owned)
    return (shrunk, shrinkage.reshape(()), carried[:NF].reshape(block))


def solution(mesh):
    finer = Mesh(mesh.devices.reshape(NY, NZ, NX, NC), EVERY)
    return jax.shard_map(
        shrinkage_step,
        mesh=finer,
        in_specs=(P(EVERY, None),),
        out_specs=(P(PLANE, LINE), P(), P(LINE)),
        check_vma=False,
    )
```

```python
import functools

import jax
import jax.numpy as jnp
from jax import lax
from jax.experimental import pallas as pl
from jax.experimental.pallas import tpu as pltpu
from jax.sharding import Mesh
from jax.sharding import PartitionSpec as P


PLANE = ("y", "z")
LINE = ("x", "c")
SLAB = ("z", "x", "c")
EVERY = ("y", "z", "x", "c")
F32 = jnp.float32
BF16 = jnp.bfloat16
LANES = 128
NY, NZ, NX, NC = 8, 8, 4, 2
NF = NX * NC
SHIFT = (0, 4, 1, 7, 2, 6, 3, 5)
COLUMN = tuple(2 * (z % 4) + z // 4 for z in range(NZ))
HOLDER = tuple(COLUMN.index(block) for block in range(NZ))
OFF, SECOND, MEANS = 64, 65, 66
F16 = jnp.float16
IN_VMEM = pl.BlockSpec(memory_space=pltpu.VMEM)
IN_SMEM = pl.BlockSpec(memory_space=pltpu.SMEM)


def deal_kernel(core_ref, x_ref, out_ref):
    block = out_ref.shape[3]

    def deal(core):
        order = [2 * x + core for x in range(NX)] + [2 * x + 1 - core for x in range(NX)]
        for b in range(NY):
            whole = x_ref[:, b * block : (b + 1) * block]
            cuts = [whole[:, k * LANES : (k + 1) * LANES] for k in range(NF)]
            for z in range(NZ):
                for place, f in enumerate(order):
                    out_ref[b * NZ + z, 0, :, place * LANES : (place + 1) * LANES] = cuts[
                        (z + SHIFT[f]) % NZ
                    ]
            for y in range(NY):
                out_ref[y * NZ + HOLDER[b], 1] = whole

    for core in range(NC):
        pl.when(core_ref[0] == core)(functools.partial(deal, core))


def sums_kernel(core_ref, x_ref, told_ref):
    plane, _, rows, block = x_ref.shape
    core = core_ref[0]
    far = jnp.zeros((rows, LANES), F32)
    lines = []
    for part in range(2):
        pivot = jnp.broadcast_to(x_ref[0, part].astype(F32)[0:1], (rows, block))

        def one(p, carry):
            total, wide = carry
            value = x_ref[p, part].astype(F32)
            return total + value, jnp.maximum(wide, jnp.abs(value - pivot))

        zero = jnp.zeros((rows, block), F32)
        total, wide = lax.fori_loop(0, plane, one, (zero, zero), unroll=2)
        total = jnp.sum(total, axis=0, keepdims=True)
        for k in range(block // LANES):
            cut = slice(k * LANES, (k + 1) * LANES)
            far = jnp.maximum(far, wide[:, cut])
            lines.append(total[:, cut])
    far = jnp.max(jnp.max(far, axis=1, keepdims=True), axis=0, keepdims=True)
    dealt = jnp.concatenate(lines[:NF], axis=0)
    swapped = jnp.concatenate(lines[NX:NF] + lines[:NX], axis=0)
    plain = jnp.where(core == 0, dealt, swapped)
    out = jnp.concatenate(
        [plain] + lines[NF:] + [jnp.broadcast_to(far, (8, LANES))], axis=0
    )
    for f in range(NF):
        told_ref[f] = out


def means_kernel(core_ref, told_ref, half_ref, cols_ref, carried_ref, scale_ref, *, rows, held):
    told = told_ref[...]
    sums = told[:, : 2 * NF]
    means = jnp.sum(sums, axis=0) * (1.0 / rows)
    apart = jnp.max(jnp.abs(sums * (1.0 / held) - means[None]), axis=0)

    def top(value):
        return jnp.max(jnp.max(value, axis=1, keepdims=True), axis=0, keepdims=True)

    reach = 2.0 * top(jnp.max(told[:, 2 * NF :], axis=0)) + top(apart)
    power = half_power(reach * reach)
    mine = jnp.where(core_ref[0] == 0, means[:NX], means[NX:NF])
    for k in range(NX):
        half_ref[:, k * LANES : (k + 1) * LANES] = mine[k : k + 1]
    for k in range(NF):
        cols_ref[:, k * LANES : (k + 1) * LANES] = means[NF + k : NF + k + 1]
    up = jnp.exp2(power)
    carried_ref[...] = jnp.concatenate(
        (means[NF:], jnp.broadcast_to(up, (8, LANES))), axis=0
    )
    scale_ref[...] = in_lane(0, jnp.exp2(-power) * (1.0 / rows), jnp.zeros((1, LANES), F32))


def add_all(value):
    return jnp.sum(jnp.sum(value, axis=1, keepdims=True), axis=0, keepdims=True)


def half_power(top):
    return jnp.clip(jnp.floor(jnp.log2(jnp.maximum(top, 1e-30))), -90.0, 90.0) - 13.0


def in_lane(k, value, row):
    slot = lax.broadcasted_iota(jnp.int32, (1, LANES), 1)
    return jnp.where(slot == k, value, row)


def block_kernel(place_ref, sum_ref, norms_ref, carried_ref, message_ref):
    width, block = sum_ref.shape
    lane = lax.broadcasted_iota(jnp.int32, (8, block), 1)
    sub = lax.broadcasted_iota(jnp.int32, (8, block), 0)
    first = place_ref[0]
    factor = jnp.concatenate([carried_ref[NF : NF + 8, :]] * (block // LANES), axis=1)
    zero = jnp.zeros((8, LANES), F32)
    off, diagonal = zero, zero
    for k in range(width // 8):
        tile = sum_ref[pl.ds(k * 8, 8), :] * factor
        hit = lane == first + k * 8 + sub
        rest = jnp.where(hit, 0.0, tile)
        kept = jnp.where(hit, tile, 0.0)
        squares = rest * rest
        for j in range(block // LANES):
            cut = slice(j * LANES, (j + 1) * LANES)
            off = off + squares[:, cut]
            diagonal = diagonal + kept[:, cut]
    own = lane[:, :LANES] % 8 == sub[:, :LANES]
    flag = jnp.where(first >= 0, 1.0, 0.0)
    mean = add_all(diagonal) / width
    apart = jnp.where(own, diagonal - mean, 0.0)
    row = in_lane(OFF, add_all(off), norms_ref[...])
    row = in_lane(SECOND, add_all(apart * apart) * flag, row)
    row = in_lane(MEANS, mean * flag, row)
    flags = in_lane(MEANS, flag, jnp.zeros((1, LANES), F32))
    message_ref[...] = jnp.broadcast_to(
        jnp.concatenate((row, flags), axis=0)[None], message_ref.shape
    )


def middle_kernel(seen_ref, message_ref, *, width):
    seen = seen_ref[...]
    slot = lax.broadcasted_iota(jnp.int32, (1, 1, LANES), 2)
    values, flags = seen[:, 0:1, :], seen[:, 1:2, :]
    norms = jnp.sum(values.reshape(NZ, NF, 1, LANES), axis=0)
    norms = jnp.where(slot < OFF, norms, 0.0)
    total = jnp.sum(values, axis=0)
    is_mean = slot == MEANS

    def lanes(row):
        return jnp.sum(row, axis=1, keepdims=True)

    mean = lanes(jnp.where(is_mean[0], total, 0.0)) / NF
    apart = jnp.where(is_mean, (values - mean[None]) * flags, 0.0)
    between = lanes(jnp.sum(apart * apart, axis=0))
    second = lanes(jnp.where(slot[0] == SECOND, total, 0.0)) + width * between
    row = jnp.zeros((1, LANES), F32)
    row = in_lane(0, lanes(jnp.sum(norms, axis=0)), row)
    row = in_lane(1, lanes(jnp.sum(norms * norms, axis=0)), row)
    row = in_lane(2, lanes(jnp.where(slot[0] == OFF, total, 0.0)), row)
    row = in_lane(3, mean, row)
    row = in_lane(4, second, row)
    message_ref[...] = jnp.broadcast_to(row[None], message_ref.shape)


def shrink_kernel(
    place_ref, carried_ref, totals_ref, owned_ref, shrunk_ref, value_ref, mean_ref, *, rows, factors
):
    width, block = shrunk_ref.shape
    first = place_ref[0]
    slot = lax.broadcasted_iota(jnp.int32, (1, LANES), 1)
    totals = totals_ref[...]
    sums = jnp.sum(totals, axis=0)

    def pick(row, k):
        return jnp.sum(jnp.where(slot == k, row, 0.0), axis=1, keepdims=True)

    mu_scale = pick(sums, 0) / (rows * factors)
    apart = totals - mu_scale[None]
    from_mu = pick(jnp.sum(apart * apart, axis=0), 3)
    spread = (pick(sums, 2) + pick(sums, 4) + block * from_mu) / factors
    norm_sq = factors * (spread + mu_scale * mu_scale)
    beta_value = (pick(sums, 1) / rows - norm_sq) / (factors * rows)
    shrinkage = beta_value / spread
    value_ref[...] = shrinkage
    mean_ref[...] = carried_ref[:NF, :]
    keep = (1.0 - shrinkage) * carried_ref[NF : NF + 1, 0:1]
    lift = shrinkage * mu_scale
    lane = lax.broadcasted_iota(jnp.int32, (8, block), 1)
    sub = lax.broadcasted_iota(jnp.int32, (8, block), 0)
    for k in range(width // 8):
        at = pl.ds(k * 8, 8)
        hit = lane == first + k * 8 + sub
        shrunk_ref[at, :] = keep * owned_ref[at, :] + jnp.where(hit, lift, 0.0)


def in_vmem(value):
    return pltpu.with_memory_space_constraint(value, pltpu.VMEM)


def flip(size):
    return [(k, k ^ 1) for k in range(size)]


def product(left, right):
    return lax.dot_general(left, right, (((0,), (0,)), ((), ())), preferred_element_type=F32)


def shrinkage_step(scenarios):
    row_count, factors = scenarios.shape
    plane = NY * NZ
    total_rows = row_count * plane * NF
    part_rows = row_count * plane
    block = factors // NY
    half, width = block // 2, block // NF
    y_idx, z_idx = lax.axis_index("y"), lax.axis_index("z")
    x_idx, c_idx = lax.axis_index("x"), lax.axis_index("c")
    f_idx = x_idx * NC + c_idx
    exchange = functools.partial(lax.all_to_all, split_axis=0, concat_axis=0, tiled=True)
    shapes = jax.ShapeDtypeStruct

    core = c_idx.reshape(1)
    dealt = pl.pallas_call(
        deal_kernel,
        out_shape=pltpu.VMEM((plane, 2, row_count, block), BF16),
        in_specs=[IN_SMEM, IN_VMEM],
        out_specs=IN_VMEM,
        name="deal",
    )(core, scenarios)
    arrived = exchange(dealt, PLANE)

    swapped = lax.ppermute(arrived, "c", flip(NC))
    told = pl.pallas_call(
        sums_kernel,
        out_shape=pltpu.VMEM((NF, 3 * NF, LANES), F32),
        in_specs=[IN_SMEM, IN_VMEM],
        out_specs=IN_VMEM,
        name="sums",
    )(core, in_vmem(arrived))
    told = exchange(told, LINE)
    mean_half, mean_c, carried, scale = pl.pallas_call(
        functools.partial(means_kernel, rows=total_rows, held=part_rows),
        out_shape=(
            pltpu.VMEM((1, half), F32),
            pltpu.VMEM((1, block), F32),
            pltpu.VMEM((2 * NF, LANES), F32),
            pltpu.VMEM((1, LANES), F32),
        ),
        in_specs=[IN_SMEM, IN_VMEM],
        out_specs=(IN_VMEM,) * 4,
        name="means",
    )(core, in_vmem(told))

    def centred(rows, mean):
        out = (rows.astype(F32) - mean).astype(BF16)
        return out.reshape(part_rows, out.shape[-1])

    partial = product(centred(arrived[:, 0, :, :half], mean_half), centred(arrived[:, 1], mean_c))
    partial = partial + product(
        centred(swapped[:, 0, :, half:], mean_half), centred(swapped[:, 1], mean_c)
    )
    parcel = (partial * scale[0, 0]).astype(F16)
    pieces = exchange(parcel.reshape(NX, width, block), "x")
    summed = jnp.sum(pieces.astype(F32), axis=0)

    mine = lax.dynamic_slice_in_dim(arrived, y_idx * NZ, NZ, 0)[:, 1]
    mine = (mine.astype(F32) - mean_c).astype(BF16).astype(F32)
    norms = jnp.sum(mine * mine, axis=2).reshape(1, NZ * row_count)
    norms = jnp.pad(norms, ((0, 0), (0, LANES - NZ * row_count)))

    shift = jnp.array(SHIFT, jnp.int32)[f_idx]
    column = 2 * (z_idx % 4) + z_idx // 4
    never = -2 * block
    first = jnp.where(y_idx == column, (z_idx + shift) % NZ * width, never)
    message = pl.pallas_call(
        block_kernel,
        out_shape=pltpu.VMEM((NZ * NF, 2, LANES), F32),
        in_specs=[IN_SMEM, IN_VMEM, IN_VMEM, IN_VMEM],
        out_specs=IN_VMEM,
        name="block_stats",
    )(first.reshape(1), in_vmem(summed), in_vmem(norms), in_vmem(carried))

    seen = exchange(message, SLAB)

    def owner(z, f):
        return ((z + SHIFT[f]) % NZ) * NF + COLUMN[z]

    moves = [(z * NF + f, owner(z, f)) for z in range(NZ) for f in range(NF)]
    owned = lax.ppermute(summed.astype(F16), SLAB, moves).astype(F32)
    carried = lax.ppermute(carried, SLAB, moves)
    second = pl.pallas_call(
        functools.partial(middle_kernel, width=width),
        out_shape=pltpu.VMEM((NY, 1, LANES), F32),
        in_specs=[IN_VMEM],
        out_specs=IN_VMEM,
        name="middle_stats",
    )(in_vmem(seen))
    totals = exchange(second, "y")

    first_own = jnp.where(y_idx == f_idx, z_idx * width, never)
    shrunk, shrinkage, col_mean = pl.pallas_call(
        functools.partial(shrink_kernel, rows=total_rows, factors=factors),
        out_shape=(
            shapes((width, block), F32),
            shapes((1, 1), F32),
            shapes((NF, LANES), F32),
        ),
        in_specs=[IN_SMEM, IN_VMEM, IN_VMEM, IN_VMEM],
        out_specs=(IN_VMEM, IN_VMEM, IN_VMEM),
        name="shrink",
    )(first_own.reshape(1), in_vmem(carried), in_vmem(totals), in_vmem(owned))
    return (shrunk, shrinkage.reshape(()), col_mean.reshape(block))


def solution(mesh):
    finer = Mesh(mesh.devices.reshape(NY, NZ, NX, NC), EVERY)
    return jax.shard_map(
        shrinkage_step,
        mesh=finer,
        in_specs=(P(EVERY, None),),
        out_specs=(P(PLANE, LINE), P(), P(LINE)),
        check_vma=False,
    )
```

```python
import functools

import jax
import jax.numpy as jnp
from jax import lax
from jax.experimental import pallas as pl
from jax.experimental.pallas import tpu as pltpu
from jax.sharding import Mesh
from jax.sharding import PartitionSpec as P


PLANE = ("y", "z")
LINE = ("x", "c")
SLAB = ("z", "x", "c")
EVERY = ("y", "z", "x", "c")
F32 = jnp.float32
BF16 = jnp.bfloat16
LANES = 128
NY, NZ, NX, NC = 8, 8, 4, 2
NF = NX * NC
SHIFT = (0, 4, 1, 7, 2, 6, 3, 5)
COLUMN = tuple(2 * (z % 4) + z // 4 for z in range(NZ))
HOLDER = tuple(COLUMN.index(block) for block in range(NZ))
OFF, SECOND, MEANS = 64, 65, 66
F16 = jnp.float16
IN_VMEM = pl.BlockSpec(memory_space=pltpu.VMEM)
IN_SMEM = pl.BlockSpec(memory_space=pltpu.SMEM)


def deal_kernel(core_ref, x_ref, out_ref):
    block = out_ref.shape[3]

    def deal(core):
        order = [2 * x + core for x in range(NX)] + [2 * x + 1 - core for x in range(NX)]
        for b in range(NY):
            whole = x_ref[:, b * block : (b + 1) * block]
            cuts = [whole[:, k * LANES : (k + 1) * LANES] for k in range(NF)]
            for z in range(NZ):
                for place, f in enumerate(order):
                    out_ref[b * NZ + z, 0, :, place * LANES : (place + 1) * LANES] = cuts[
                        (z + SHIFT[f]) % NZ
                    ]
            for y in range(NY):
                out_ref[y * NZ + HOLDER[b], 1] = whole

    for core in range(NC):
        pl.when(core_ref[0] == core)(functools.partial(deal, core))


def sums_kernel(core_ref, x_ref, told_ref):
    _, _, _, block = x_ref.shape
    far = jnp.zeros((1, LANES), F32)
    lines = []
    for part in range(2):
        for k in range(block // LANES):
            at = slice(k * LANES, (k + 1) * LANES)
            value = x_ref[:, part, :, at]
            line = jnp.sum(jnp.sum(value.astype(F32), axis=0), axis=0, keepdims=True)
            high = jnp.max(jnp.max(value, axis=0).astype(F32), axis=0, keepdims=True)
            low = jnp.min(jnp.min(value, axis=0).astype(F32), axis=0, keepdims=True)
            far = jnp.maximum(far, high - low)
            lines.append(line)
    far = jnp.max(far, axis=1, keepdims=True)
    dealt = jnp.concatenate(lines[:NF], axis=0)
    swapped = jnp.concatenate(lines[NX:NF] + lines[:NX], axis=0)
    plain = jnp.where(core_ref[0] == 0, dealt, swapped)
    out = jnp.concatenate(
        [plain] + lines[NF:] + [jnp.broadcast_to(far, (8, LANES))], axis=0
    )
    for f in range(NF):
        told_ref[f] = out


def means_kernel(core_ref, told_ref, half_ref, cols_ref, carried_ref, scale_ref, *, rows, held):
    told = told_ref[...]
    sums = told[:, : 2 * NF]
    means = jnp.sum(sums, axis=0) * (1.0 / rows)
    apart = jnp.max(jnp.abs(sums * (1.0 / held) - means[None]), axis=0)

    def top(value):
        return jnp.max(jnp.max(value, axis=1, keepdims=True), axis=0, keepdims=True)

    reach = top(jnp.max(told[:, 2 * NF :], axis=0)) + top(apart)
    power = half_power(reach * reach)
    mine = jnp.where(core_ref[0] == 0, means[:NX], means[NX:NF])
    for k in range(NX):
        half_ref[:, k * LANES : (k + 1) * LANES] = mine[k : k + 1]
    for k in range(NF):
        cols_ref[:, k * LANES : (k + 1) * LANES] = means[NF + k : NF + k + 1]
    up = jnp.exp2(power)
    carried_ref[...] = jnp.concatenate(
        (means[NF:], jnp.broadcast_to(up, (8, LANES))), axis=0
    )
    scale_ref[...] = in_lane(0, jnp.exp2(-power) * (1.0 / rows), jnp.zeros((1, LANES), F32))


def add_all(value):
    return jnp.sum(jnp.sum(value, axis=1, keepdims=True), axis=0, keepdims=True)


def half_power(top):
    return jnp.clip(jnp.floor(jnp.log2(jnp.maximum(top, 1e-30))), -90.0, 90.0) - 13.0


def in_lane(k, value, row):
    slot = lax.broadcasted_iota(jnp.int32, (1, LANES), 1)
    return jnp.where(slot == k, value, row)


def block_kernel(place_ref, sum_ref, norms_ref, carried_ref, message_ref):
    width, block = sum_ref.shape
    lane = lax.broadcasted_iota(jnp.int32, (8, block), 1)
    sub = lax.broadcasted_iota(jnp.int32, (8, block), 0)
    first = place_ref[0]
    factor = jnp.concatenate([carried_ref[NF : NF + 8, :]] * (block // LANES), axis=1)
    zero = jnp.zeros((8, LANES), F32)
    off, diagonal = zero, zero
    for k in range(width // 8):
        tile = sum_ref[pl.ds(k * 8, 8), :] * factor
        hit = lane == first + k * 8 + sub
        rest = jnp.where(hit, 0.0, tile)
        kept = jnp.where(hit, tile, 0.0)
        squares = rest * rest
        for j in range(block // LANES):
            cut = slice(j * LANES, (j + 1) * LANES)
            off = off + squares[:, cut]
            diagonal = diagonal + kept[:, cut]
    own = lane[:, :LANES] % 8 == sub[:, :LANES]
    flag = jnp.where(first >= 0, 1.0, 0.0)
    mean = add_all(diagonal) / width
    apart = jnp.where(own, diagonal - mean, 0.0)
    row = in_lane(OFF, add_all(off), norms_ref[...])
    row = in_lane(SECOND, add_all(apart * apart) * flag, row)
    row = in_lane(MEANS, mean * flag, row)
    flags = in_lane(MEANS, flag, jnp.zeros((1, LANES), F32))
    message_ref[...] = jnp.broadcast_to(
        jnp.concatenate((row, flags), axis=0)[None], message_ref.shape
    )


def middle_kernel(seen_ref, message_ref, *, width):
    seen = seen_ref[...]
    slot = lax.broadcasted_iota(jnp.int32, (1, 1, LANES), 2)
    values, flags = seen[:, 0:1, :], seen[:, 1:2, :]
    norms = jnp.sum(values.reshape(NZ, NC, 1, LANES), axis=0)
    norms = jnp.where(slot < OFF, norms, 0.0)
    total = jnp.sum(values, axis=0)
    is_mean = slot == MEANS

    def lanes(row):
        return jnp.sum(row, axis=1, keepdims=True)

    mean = lanes(jnp.where(is_mean[0], total, 0.0)) / NC
    apart = jnp.where(is_mean, (values - mean[None]) * flags, 0.0)
    between = lanes(jnp.sum(apart * apart, axis=0))
    second = lanes(jnp.where(slot[0] == SECOND, total, 0.0)) + width * between
    row = jnp.zeros((1, LANES), F32)
    row = in_lane(0, lanes(jnp.sum(norms, axis=0)), row)
    row = in_lane(1, lanes(jnp.sum(norms * norms, axis=0)), row)
    row = in_lane(2, lanes(jnp.where(slot[0] == OFF, total, 0.0)), row)
    row = in_lane(3, mean, row)
    row = in_lane(4, second, row)
    message_ref[...] = jnp.broadcast_to(row[None], message_ref.shape)


def shrink_kernel(
    place_ref, carried_ref, totals_ref, owned_ref, shrunk_ref, value_ref, mean_ref, *, rows, factors
):
    width, block = shrunk_ref.shape
    first = place_ref[0]
    slot = lax.broadcasted_iota(jnp.int32, (1, LANES), 1)
    totals = totals_ref[...]
    sums = jnp.sum(totals, axis=0)

    def pick(row, k):
        return jnp.sum(jnp.where(slot == k, row, 0.0), axis=1, keepdims=True)

    mu_scale = pick(sums, 0) / (rows * factors)
    apart = totals - mu_scale[None]
    from_mu = pick(jnp.sum(apart * apart, axis=0), 3)
    spread = (pick(sums, 2) + pick(sums, 4) + NC * width * from_mu) / factors
    norm_sq = factors * (spread + mu_scale * mu_scale)
    beta_value = (pick(sums, 1) / rows - norm_sq) / (factors * rows)
    shrinkage = beta_value / spread
    value_ref[...] = shrinkage
    mean_ref[...] = carried_ref[:NF, :]
    keep = (1.0 - shrinkage) * carried_ref[NF : NF + 1, 0:1]
    lift = shrinkage * mu_scale
    lane = lax.broadcasted_iota(jnp.int32, (8, block), 1)
    sub = lax.broadcasted_iota(jnp.int32, (8, block), 0)
    for k in range(width // 8):
        at = pl.ds(k * 8, 8)
        hit = lane == first + k * 8 + sub
        shrunk_ref[at, :] = keep * owned_ref[at, :] + jnp.where(hit, lift, 0.0)


def in_vmem(value):
    return pltpu.with_memory_space_constraint(value, pltpu.VMEM)


def flip(size):
    return [(k, k ^ 1) for k in range(size)]


def product(left, right):
    return lax.dot_general(left, right, (((0,), (0,)), ((), ())), preferred_element_type=F32)


def shrinkage_step(scenarios):
    row_count, factors = scenarios.shape
    plane = NY * NZ
    total_rows = row_count * plane * NF
    part_rows = row_count * plane
    block = factors // NY
    half, width = block // 2, block // NF
    y_idx, z_idx = lax.axis_index("y"), lax.axis_index("z")
    x_idx, c_idx = lax.axis_index("x"), lax.axis_index("c")
    f_idx = x_idx * NC + c_idx
    exchange = functools.partial(lax.all_to_all, split_axis=0, concat_axis=0, tiled=True)
    shapes = jax.ShapeDtypeStruct

    core = c_idx.reshape(1)
    dealt = pl.pallas_call(
        deal_kernel,
        out_shape=pltpu.VMEM((plane, 2, row_count, block), BF16),
        in_specs=[IN_SMEM, IN_VMEM],
        out_specs=IN_VMEM,
        name="deal",
    )(core, scenarios)
    arrived = exchange(dealt, PLANE)

    swapped = lax.ppermute(arrived, "c", flip(NC))
    told = pl.pallas_call(
        sums_kernel,
        out_shape=pltpu.VMEM((NF, 3 * NF, LANES), F32),
        in_specs=[IN_SMEM, IN_VMEM],
        out_specs=IN_VMEM,
        name="sums",
    )(core, in_vmem(arrived))
    told = exchange(told, LINE)
    mean_half, mean_c, carried, scale = pl.pallas_call(
        functools.partial(means_kernel, rows=total_rows, held=part_rows),
        out_shape=(
            pltpu.VMEM((1, half), F32),
            pltpu.VMEM((1, block), F32),
            pltpu.VMEM((2 * NF, LANES), F32),
            pltpu.VMEM((1, LANES), F32),
        ),
        in_specs=[IN_SMEM, IN_VMEM],
        out_specs=(IN_VMEM,) * 4,
        name="means",
    )(core, in_vmem(told))

    def centred(rows, mean):
        out = (rows.astype(F32) - mean).astype(BF16)
        return out.reshape(part_rows, out.shape[-1])

    partial = product(centred(arrived[:, 0, :, :half], mean_half), centred(arrived[:, 1], mean_c))
    partial = partial + product(
        centred(swapped[:, 0, :, half:], mean_half), centred(swapped[:, 1], mean_c)
    )
    parcel = (partial * scale[0, 0]).astype(F16)
    pieces = exchange(parcel.reshape(NX, width, block), "x")
    summed = jnp.sum(pieces.astype(F32), axis=0)

    mine = lax.dynamic_slice_in_dim(arrived, y_idx * NZ, NZ, 0)[:, 1]
    mine = (mine.astype(F32) - mean_c).astype(BF16).astype(F32)
    norms = jnp.sum(mine * mine, axis=2).reshape(1, NZ * row_count)
    norms = jnp.pad(norms, ((0, 0), (0, LANES - NZ * row_count)))

    shift = jnp.array(SHIFT, jnp.int32)[f_idx]
    column = 2 * (z_idx % 4) + z_idx // 4
    never = -2 * block
    first = jnp.where(y_idx == column, (z_idx + shift) % NZ * width, never)
    message = pl.pallas_call(
        block_kernel,
        out_shape=pltpu.VMEM((NZ * NC, 2, LANES), F32),
        in_specs=[IN_SMEM, IN_VMEM, IN_VMEM, IN_VMEM],
        out_specs=IN_VMEM,
        name="block_stats",
    )(first.reshape(1), in_vmem(summed), in_vmem(norms), in_vmem(carried))

    seen = exchange(message, ("z", "c"))

    def owner(z, f):
        return ((z + SHIFT[f]) % NZ) * NF + COLUMN[z]

    moves = [(z * NF + f, owner(z, f)) for z in range(NZ) for f in range(NF)]
    owned = lax.ppermute(summed.astype(F16), SLAB, moves).astype(F32)
    carried = lax.ppermute(carried, SLAB, moves)
    second = pl.pallas_call(
        functools.partial(middle_kernel, width=width),
        out_shape=pltpu.VMEM((NY * NX, 1, LANES), F32),
        in_specs=[IN_VMEM],
        out_specs=IN_VMEM,
        name="middle_stats",
    )(in_vmem(seen))
    totals = exchange(second, ("y", "x"))

    first_own = jnp.where(y_idx == f_idx, z_idx * width, never)
    shrunk, shrinkage, col_mean = pl.pallas_call(
        functools.partial(shrink_kernel, rows=total_rows, factors=factors),
        out_shape=(
            shapes((width, block), F32),
            shapes((1, 1), F32),
            shapes((NF, LANES), F32),
        ),
        in_specs=[IN_SMEM, IN_VMEM, IN_VMEM, IN_VMEM],
        out_specs=(IN_VMEM, IN_VMEM, IN_VMEM),
        name="shrink",
    )(first_own.reshape(1), in_vmem(carried), in_vmem(totals), in_vmem(owned))
    return (shrunk, shrinkage.reshape(()), col_mean.reshape(block))


def solution(mesh):
    finer = Mesh(mesh.devices.reshape(NY, NZ, NX, NC), EVERY)
    return jax.shard_map(
        shrinkage_step,
        mesh=finer,
        in_specs=(P(EVERY, None),),
        out_specs=(P(PLANE, LINE), P(), P(LINE)),
        check_vma=False,
    )
```

```python
import functools

import jax
import jax.numpy as jnp
from jax import lax
from jax.experimental import pallas as pl
from jax.experimental.pallas import tpu as pltpu
from jax.sharding import Mesh
from jax.sharding import PartitionSpec as P


PLANE = ("y", "z")
LINE = ("x", "c")
SLAB = ("z", "x", "c")
EVERY = ("y", "z", "x", "c")
F32 = jnp.float32
BF16 = jnp.bfloat16
LANES = 128
NY, NZ, NX, NC = 8, 8, 4, 2
NF = NX * NC
SHIFT = (0, 4, 1, 7, 2, 6, 3, 5)
COLUMN = tuple(2 * (z % 4) + z // 4 for z in range(NZ))
OFF, SECOND, MEAN = range(3)
F16 = jnp.float16
IN_VMEM = pl.BlockSpec(memory_space=pltpu.VMEM)
IN_SMEM = pl.BlockSpec(memory_space=pltpu.SMEM)


def deal_kernel(core_ref, x_ref, out_ref):
    block = out_ref.shape[3]
    each = out_ref.shape[0] // NZ
    step = pl.program_id(0)

    def deal(core):
        order = [2 * x + core for x in range(NX)] + [2 * x + 1 - core for x in range(NX)]
        for j in range(each):
            start = pl.multiple_of((step * each + j) * block, block)
            cuts = [x_ref[:, pl.ds(start + k * LANES, LANES)] for k in range(NF)]
            for z in range(NZ):
                for place, f in enumerate(order):
                    out_ref[j * NZ + z, 0, :, place * LANES : (place + 1) * LANES] = cuts[
                        (z + SHIFT[f]) % NZ
                    ]

    for core in range(NC):
        pl.when(core_ref[0] == core)(functools.partial(deal, core))
    for z in range(NZ):
        whole = x_ref[:, COLUMN[z] * block : (COLUMN[z] + 1) * block]
        for j in range(each):
            out_ref[j * NZ + z, 1] = whole


def tell_kernel(core_ref, sums_ref, wide_ref, told_ref):
    far = jnp.max(wide_ref[...], axis=1, keepdims=True)
    far = 2.0 * jnp.max(far, axis=0, keepdims=True)
    lines = [
        sums_ref[part : part + 1, k * LANES : (k + 1) * LANES] for part in range(2) for k in range(NF)
    ]
    dealt = jnp.concatenate(lines[:NF], axis=0)
    swapped = jnp.concatenate(lines[NX:NF] + lines[:NX], axis=0)
    plain = jnp.where(core_ref[0] == 0, dealt, swapped)
    out = jnp.concatenate(
        [plain] + lines[NF:] + [jnp.broadcast_to(far, (8, LANES))], axis=0
    )
    for f in range(NF):
        told_ref[f] = out


def means_kernel(core_ref, told_ref, half_ref, cols_ref, carried_ref, scale_ref, *, rows, held):
    told = told_ref[...]
    sums = told[:, : 2 * NF]
    means = jnp.sum(sums, axis=0) * (1.0 / rows)
    apart = jnp.max(jnp.abs(sums * (1.0 / held) - means[None]), axis=0)

    def top(value):
        return jnp.max(jnp.max(value, axis=1, keepdims=True), axis=0, keepdims=True)

    reach = top(jnp.max(told[:, 2 * NF :], axis=0)) + top(apart)
    power = half_power(reach * reach)
    mine = jnp.where(core_ref[0] == 0, means[:NX], means[NX:NF])
    for k in range(NX):
        half_ref[:, k * LANES : (k + 1) * LANES] = mine[k : k + 1]
    for k in range(NF):
        cols_ref[:, k * LANES : (k + 1) * LANES] = means[NF + k : NF + k + 1]
    up = jnp.exp2(power)
    carried_ref[...] = jnp.concatenate(
        (means[NF:], jnp.broadcast_to(up, (8, LANES))), axis=0
    )
    scale_ref[...] = in_lane(0, jnp.exp2(-power) * (1.0 / rows), jnp.zeros((1, LANES), F32))


def add_all(value):
    return jnp.sum(jnp.sum(value, axis=1, keepdims=True), axis=0, keepdims=True)


def half_power(top):
    return jnp.clip(jnp.floor(jnp.log2(jnp.maximum(top, 1e-30))), -90.0, 90.0) - 13.0


def in_lane(k, value, row):
    slot = lax.broadcasted_iota(jnp.int32, (1, LANES), 1)
    return jnp.where(slot == k, value, row)


def block_kernel(place_ref, sum_ref, carried_ref, message_ref):
    width, block = sum_ref.shape
    lane = lax.broadcasted_iota(jnp.int32, (8, block), 1)
    sub = lax.broadcasted_iota(jnp.int32, (8, block), 0)
    first = place_ref[0]
    factor = jnp.concatenate([carried_ref[NF : NF + 8, :]] * (block // LANES), axis=1)
    zero = jnp.zeros((8, LANES), F32)
    off, diagonal = zero, zero
    for k in range(width // 8):
        tile = sum_ref[pl.ds(k * 8, 8), :] * factor
        hit = lane == first + k * 8 + sub
        rest = jnp.where(hit, 0.0, tile)
        kept = jnp.where(hit, tile, 0.0)
        squares = rest * rest
        for j in range(block // LANES):
            cut = slice(j * LANES, (j + 1) * LANES)
            off = off + squares[:, cut]
            diagonal = diagonal + kept[:, cut]
    own = lane[:, :LANES] % 8 == sub[:, :LANES]
    flag = jnp.where(first >= 0, 1.0, 0.0)
    mean = add_all(diagonal) / width
    apart = jnp.where(own, diagonal - mean, 0.0)
    row = in_lane(OFF, add_all(off), jnp.zeros((1, LANES), F32))
    row = in_lane(SECOND, add_all(apart * apart) * flag, row)
    row = in_lane(MEAN, mean * flag, row)
    message_ref[...] = jnp.broadcast_to(row[None], message_ref.shape)


def middle_kernel(seen_ref, norms_ref, message_ref):
    row = jnp.sum(seen_ref[...], axis=0)
    message_ref[...] = jnp.broadcast_to(
        jnp.concatenate((norms_ref[...], row), axis=0)[None], message_ref.shape
    )


def shrink_kernel(
    place_ref, carried_ref, totals_ref, owned_ref, shrunk_ref, value_ref, mean_ref, *, rows, factors
):
    width, block = shrunk_ref.shape
    first = place_ref[0]
    slot = lax.broadcasted_iota(jnp.int32, (1, LANES), 1)
    lines = totals_ref.shape[1] - 1
    norms = jnp.sum(totals_ref[:, :lines].reshape(NZ, NF, lines, LANES), axis=0)
    trace_total = add_all(jnp.sum(norms, axis=0))
    fourth_total = add_all(jnp.sum(norms * norms, axis=0))
    scalars = totals_ref[:, lines:]
    sums = jnp.sum(scalars, axis=0)

    def pick(row, k):
        return jnp.sum(jnp.where(slot == k, row, 0.0), axis=1, keepdims=True)

    mu_scale = trace_total / (rows * factors)
    apart = scalars - mu_scale[None]
    from_mu = pick(jnp.sum(apart * apart, axis=0), MEAN)
    spread = (pick(sums, OFF) + pick(sums, SECOND) + width * from_mu) / factors
    norm_sq = factors * (spread + mu_scale * mu_scale)
    beta_value = (fourth_total / rows - norm_sq) / (factors * rows)
    shrinkage = beta_value / spread
    value_ref[...] = shrinkage
    mean_ref[...] = carried_ref[:NF, :]
    keep = (1.0 - shrinkage) * carried_ref[NF : NF + 1, 0:1]
    lift = shrinkage * mu_scale
    lane = lax.broadcasted_iota(jnp.int32, (8, block), 1)
    sub = lax.broadcasted_iota(jnp.int32, (8, block), 0)
    for k in range(width // 8):
        at = pl.ds(k * 8, 8)
        hit = lane == first + k * 8 + sub
        shrunk_ref[at, :] = keep * owned_ref[at, :] + jnp.where(hit, lift, 0.0)


def in_vmem(value):
    return pltpu.with_memory_space_constraint(value, pltpu.VMEM)


def flip(size):
    return [(k, k ^ 1) for k in range(size)]


def product(left, right):
    return lax.dot_general(left, right, (((0,), (0,)), ((), ())), preferred_element_type=F32)


def shrinkage_step(scenarios):
    row_count, factors = scenarios.shape
    plane = NY * NZ
    total_rows = row_count * plane * NF
    part_rows = row_count * plane
    block = factors // NY
    half, width = block // 2, block // NF
    y_idx, z_idx = lax.axis_index("y"), lax.axis_index("z")
    x_idx, c_idx = lax.axis_index("x"), lax.axis_index("c")
    f_idx = x_idx * NC + c_idx
    exchange = functools.partial(lax.all_to_all, split_axis=0, concat_axis=0, tiled=True)
    shapes = jax.ShapeDtypeStruct

    core = c_idx.reshape(1)
    steps = 4
    dealt = pl.pallas_call(
        deal_kernel,
        grid=(steps,),
        out_shape=shapes((plane, 2, row_count, block), BF16),
        in_specs=[IN_SMEM, IN_VMEM],
        out_specs=pl.BlockSpec((plane // steps, 2, row_count, block), lambda i: (i, 0, 0, 0)),
        name="deal",
    )(core, scenarios)
    arrived = exchange(dealt, PLANE)

    swapped = lax.ppermute(arrived, "c", flip(NC))
    values = arrived.astype(F32)
    sums = jnp.sum(values, axis=(0, 2))
    wide = jnp.max(jnp.abs(values - values[:1, :, :1]), axis=(0, 2))
    told = pl.pallas_call(
        tell_kernel,
        out_shape=shapes((NF, 3 * NF, LANES), F32),
        in_specs=[IN_SMEM, IN_VMEM, IN_VMEM],
        out_specs=IN_VMEM,
        name="tell",
    )(core, in_vmem(sums), in_vmem(wide))
    told = exchange(told, LINE)
    mean_half, mean_c, carried, scale = pl.pallas_call(
        functools.partial(means_kernel, rows=total_rows, held=part_rows),
        out_shape=(
            pltpu.VMEM((1, half), F32),
            pltpu.VMEM((1, block), F32),
            pltpu.VMEM((2 * NF, LANES), F32),
            pltpu.VMEM((1, LANES), F32),
        ),
        in_specs=[IN_SMEM, IN_VMEM],
        out_specs=(IN_VMEM,) * 4,
        name="means",
    )(core, in_vmem(told))

    def centred(rows, mean):
        out = (rows.astype(F32) - mean).astype(BF16)
        return out.reshape(part_rows, out.shape[-1])

    partial = product(centred(arrived[:, 0, :, :half], mean_half), centred(arrived[:, 1], mean_c))
    partial = partial + product(
        centred(swapped[:, 0, :, half:], mean_half), centred(swapped[:, 1], mean_c)
    )
    parcel = (partial * scale[0, 0]).astype(F16)
    pieces = exchange(parcel.reshape(NX, width, block), "x")
    summed = jnp.sum(pieces.astype(F32), axis=0)

    mine = (arrived[:, 1].astype(F32) - mean_c).astype(BF16).astype(F32)
    norms = jnp.sum(mine * mine, axis=2).reshape(part_rows // LANES, LANES)

    shift = jnp.array(SHIFT, jnp.int32)[f_idx]
    column = 2 * (z_idx % 4) + z_idx // 4
    never = -2 * block
    first = jnp.where(y_idx == column, (z_idx + shift) % NZ * width, never)
    message = pl.pallas_call(
        block_kernel,
        out_shape=shapes((NY, 1, LANES), F32),
        in_specs=[IN_SMEM, IN_VMEM, IN_VMEM],
        out_specs=IN_VMEM,
        name="block_stats",
    )(first.reshape(1), in_vmem(summed), in_vmem(carried))

    seen = exchange(message, "y")

    def owner(z, f):
        return ((z + SHIFT[f]) % NZ) * NF + COLUMN[z]

    moves = [(z * NF + f, owner(z, f)) for z in range(NZ) for f in range(NF)]
    owned = lax.ppermute(summed.astype(F16), SLAB, moves).astype(F32)
    carried = lax.ppermute(carried, SLAB, moves)
    second = pl.pallas_call(
        middle_kernel,
        out_shape=shapes((NZ * NF, part_rows // LANES + 1, LANES), F32),
        in_specs=[IN_VMEM, IN_VMEM],
        out_specs=IN_VMEM,
        name="middle_stats",
    )(in_vmem(seen), in_vmem(norms))
    totals = exchange(second, SLAB)

    first_own = jnp.where(y_idx == f_idx, z_idx * width, never)
    shrunk, shrinkage, col_mean = pl.pallas_call(
        functools.partial(shrink_kernel, rows=total_rows, factors=factors),
        out_shape=(
            shapes((width, block), F32),
            shapes((1, 1), F32),
            shapes((NF, LANES), F32),
        ),
        in_specs=[IN_SMEM, IN_VMEM, IN_VMEM, IN_VMEM],
        out_specs=(IN_VMEM, IN_VMEM, IN_VMEM),
        name="shrink",
    )(first_own.reshape(1), in_vmem(carried), in_vmem(totals), in_vmem(owned))
    return (shrunk, shrinkage.reshape(()), col_mean.reshape(block))


def solution(mesh):
    finer = Mesh(mesh.devices.reshape(NY, NZ, NX, NC), EVERY)
    return jax.shard_map(
        shrinkage_step,
        mesh=finer,
        in_specs=(P(EVERY, None),),
        out_specs=(P(PLANE, LINE), P(), P(LINE)),
        check_vma=False,
    )
```

```python
import functools

import jax
import jax.numpy as jnp
from jax import lax
from jax.experimental import pallas as pl
from jax.experimental.pallas import tpu as pltpu
from jax.sharding import Mesh
from jax.sharding import PartitionSpec as P


PLANE = ("y", "z")
LINE = ("x", "c")
SLAB = ("z", "x", "c")
EVERY = ("y", "z", "x", "c")
F32 = jnp.float32
BF16 = jnp.bfloat16
LANES = 128
NY, NZ, NX, NC = 8, 8, 4, 2
NF = NX * NC
SHIFT = (0, 4, 1, 7, 2, 6, 3, 5)
COLUMN = tuple(2 * (z % 4) + z // 4 for z in range(NZ))
HOLDER = tuple(COLUMN.index(block) for block in range(NZ))
OFF, SECOND, MEANS = 64, 65, 66
F16 = jnp.float16
IN_VMEM = pl.BlockSpec(memory_space=pltpu.VMEM)
IN_SMEM = pl.BlockSpec(memory_space=pltpu.SMEM)


def deal_kernel(core_ref, x_ref, out_ref):
    block = out_ref.shape[3]

    def deal(core):
        order = [2 * x + core for x in range(NX)] + [2 * x + 1 - core for x in range(NX)]
        for b in range(NY):
            whole = x_ref[:, b * block : (b + 1) * block]
            cuts = [whole[:, k * LANES : (k + 1) * LANES] for k in range(NF)]
            for z in range(NZ):
                for place, f in enumerate(order):
                    out_ref[b * NZ + z, 0, :, place * LANES : (place + 1) * LANES] = cuts[
                        (z + SHIFT[f]) % NZ
                    ]
            for y in range(NY):
                out_ref[y * NZ + HOLDER[b], 1] = whole

    for core in range(NC):
        pl.when(core_ref[0] == core)(functools.partial(deal, core))


def tell_kernel(core_ref, sums_ref, wide_ref, told_ref):
    far = jnp.max(wide_ref[...], axis=1, keepdims=True)
    far = 2.0 * jnp.max(far, axis=0, keepdims=True)
    lines = [
        sums_ref[part : part + 1, k * LANES : (k + 1) * LANES] for part in range(2) for k in range(NF)
    ]
    dealt = jnp.concatenate(lines[:NF], axis=0)
    swapped = jnp.concatenate(lines[NX:NF] + lines[:NX], axis=0)
    plain = jnp.where(core_ref[0] == 0, dealt, swapped)
    out = jnp.concatenate(
        [plain] + lines[NF:] + [jnp.broadcast_to(far, (8, LANES))], axis=0
    )
    for f in range(NF):
        told_ref[f] = out


def means_kernel(core_ref, told_ref, half_ref, cols_ref, carried_ref, scale_ref, *, rows, held):
    told = told_ref[...]
    sums = told[:, : 2 * NF]
    means = jnp.sum(sums, axis=0) * (1.0 / rows)
    apart = jnp.max(jnp.abs(sums * (1.0 / held) - means[None]), axis=0)

    def top(value):
        return jnp.max(jnp.max(value, axis=1, keepdims=True), axis=0, keepdims=True)

    reach = top(jnp.max(told[:, 2 * NF :], axis=0)) + top(apart)
    power = half_power(reach * reach)
    mine = jnp.where(core_ref[0] == 0, means[:NX], means[NX:NF])
    for k in range(NX):
        half_ref[:, k * LANES : (k + 1) * LANES] = mine[k : k + 1]
    for k in range(NF):
        cols_ref[:, k * LANES : (k + 1) * LANES] = means[NF + k : NF + k + 1]
    up = jnp.exp2(power)
    carried_ref[...] = jnp.concatenate(
        (means[NF:], jnp.broadcast_to(up, (8, LANES))), axis=0
    )
    scale_ref[...] = in_lane(0, jnp.exp2(-power) * (1.0 / rows), jnp.zeros((1, LANES), F32))


def add_all(value):
    return jnp.sum(jnp.sum(value, axis=1, keepdims=True), axis=0, keepdims=True)


def half_power(top):
    return jnp.clip(jnp.floor(jnp.log2(jnp.maximum(top, 1e-30))), -90.0, 90.0) - 13.0


def in_lane(k, value, row):
    slot = lax.broadcasted_iota(jnp.int32, (1, LANES), 1)
    return jnp.where(slot == k, value, row)


def block_kernel(place_ref, sum_ref, norms_ref, carried_ref, message_ref):
    width, block = sum_ref.shape
    lane = lax.broadcasted_iota(jnp.int32, (8, block), 1)
    sub = lax.broadcasted_iota(jnp.int32, (8, block), 0)
    first = place_ref[0]
    factor = jnp.concatenate([carried_ref[NF : NF + 8, :]] * (block // LANES), axis=1)
    zero = jnp.zeros((8, LANES), F32)
    off, diagonal = zero, zero
    for k in range(width // 8):
        tile = sum_ref[pl.ds(k * 8, 8), :] * factor
        hit = lane == first + k * 8 + sub
        rest = jnp.where(hit, 0.0, tile)
        kept = jnp.where(hit, tile, 0.0)
        squares = rest * rest
        for j in range(block // LANES):
            cut = slice(j * LANES, (j + 1) * LANES)
            off = off + squares[:, cut]
            diagonal = diagonal + kept[:, cut]
    own = lane[:, :LANES] % 8 == sub[:, :LANES]
    flag = jnp.where(first >= 0, 1.0, 0.0)
    mean = add_all(diagonal) / width
    apart = jnp.where(own, diagonal - mean, 0.0)
    row = in_lane(OFF, add_all(off), norms_ref[...])
    row = in_lane(SECOND, add_all(apart * apart) * flag, row)
    row = in_lane(MEANS, mean * flag, row)
    flags = in_lane(MEANS, flag, jnp.zeros((1, LANES), F32))
    message_ref[...] = jnp.broadcast_to(
        jnp.concatenate((row, flags), axis=0)[None], message_ref.shape
    )


def middle_kernel(seen_ref, message_ref, *, width):
    seen = seen_ref[...]
    slot = lax.broadcasted_iota(jnp.int32, (1, 1, LANES), 2)
    values, flags = seen[:, 0:1, :], seen[:, 1:2, :]
    norms = jnp.sum(values.reshape(NZ, NF, 1, LANES), axis=0)
    norms = jnp.where(slot < OFF, norms, 0.0)
    total = jnp.sum(values, axis=0)
    is_mean = slot == MEANS

    def lanes(row):
        return jnp.sum(row, axis=1, keepdims=True)

    mean = lanes(jnp.where(is_mean[0], total, 0.0)) / NF
    apart = jnp.where(is_mean, (values - mean[None]) * flags, 0.0)
    between = lanes(jnp.sum(apart * apart, axis=0))
    second = lanes(jnp.where(slot[0] == SECOND, total, 0.0)) + width * between
    row = jnp.zeros((1, LANES), F32)
    row = in_lane(0, lanes(jnp.sum(norms, axis=0)), row)
    row = in_lane(1, lanes(jnp.sum(norms * norms, axis=0)), row)
    row = in_lane(2, lanes(jnp.where(slot[0] == OFF, total, 0.0)), row)
    row = in_lane(3, mean, row)
    row = in_lane(4, second, row)
    message_ref[...] = jnp.broadcast_to(row[None], message_ref.shape)


def shrink_kernel(
    place_ref, carried_ref, totals_ref, owned_ref, shrunk_ref, value_ref, mean_ref, *, rows, factors
):
    width, block = shrunk_ref.shape
    first = place_ref[0]
    slot = lax.broadcasted_iota(jnp.int32, (1, LANES), 1)
    totals = totals_ref[...]
    sums = jnp.sum(totals, axis=0)

    def pick(row, k):
        return jnp.sum(jnp.where(slot == k, row, 0.0), axis=1, keepdims=True)

    mu_scale = pick(sums, 0) / (rows * factors)
    apart = totals - mu_scale[None]
    from_mu = pick(jnp.sum(apart * apart, axis=0), 3)
    spread = (pick(sums, 2) + pick(sums, 4) + block * from_mu) / factors
    norm_sq = factors * (spread + mu_scale * mu_scale)
    beta_value = (pick(sums, 1) / rows - norm_sq) / (factors * rows)
    shrinkage = beta_value / spread
    value_ref[...] = shrinkage
    mean_ref[...] = carried_ref[:NF, :]
    keep = (1.0 - shrinkage) * carried_ref[NF : NF + 1, 0:1]
    lift = shrinkage * mu_scale
    lane = lax.broadcasted_iota(jnp.int32, (8, block), 1)
    sub = lax.broadcasted_iota(jnp.int32, (8, block), 0)
    for k in range(width // 8):
        at = pl.ds(k * 8, 8)
        hit = lane == first + k * 8 + sub
        shrunk_ref[at, :] = keep * owned_ref[at, :] + jnp.where(hit, lift, 0.0)


def in_vmem(value):
    return pltpu.with_memory_space_constraint(value, pltpu.VMEM)


def flip(size):
    return [(k, k ^ 1) for k in range(size)]


def product(left, right):
    return lax.dot_general(left, right, (((0,), (0,)), ((), ())), preferred_element_type=F32)


def shrinkage_step(scenarios):
    row_count, factors = scenarios.shape
    plane = NY * NZ
    total_rows = row_count * plane * NF
    part_rows = row_count * plane
    block = factors // NY
    half, width = block // 2, block // NF
    y_idx, z_idx = lax.axis_index("y"), lax.axis_index("z")
    x_idx, c_idx = lax.axis_index("x"), lax.axis_index("c")
    f_idx = x_idx * NC + c_idx
    exchange = functools.partial(lax.all_to_all, split_axis=0, concat_axis=0, tiled=True)
    shapes = jax.ShapeDtypeStruct

    core = c_idx.reshape(1)
    dealt = pl.pallas_call(
        deal_kernel,
        out_shape=pltpu.VMEM((plane, 2, row_count, block), BF16),
        in_specs=[IN_SMEM, IN_VMEM],
        out_specs=IN_VMEM,
        name="deal",
    )(core, scenarios)
    arrived = exchange(dealt, PLANE)

    swapped = lax.ppermute(arrived, "c", flip(NC))
    values = arrived.astype(F32)
    sums = jnp.sum(values, axis=(0, 2))
    wide = jnp.max(jnp.abs(values - values[:1, :, :1]), axis=(0, 2))
    told = pl.pallas_call(
        tell_kernel,
        out_shape=shapes((NF, 3 * NF, LANES), F32),
        in_specs=[IN_SMEM, IN_VMEM, IN_VMEM],
        out_specs=IN_VMEM,
        name="tell",
    )(core, in_vmem(sums), in_vmem(wide))
    told = exchange(told, LINE)
    mean_half, mean_c, carried, scale = pl.pallas_call(
        functools.partial(means_kernel, rows=total_rows, held=part_rows),
        out_shape=(
            pltpu.VMEM((1, half), F32),
            pltpu.VMEM((1, block), F32),
            pltpu.VMEM((2 * NF, LANES), F32),
            pltpu.VMEM((1, LANES), F32),
        ),
        in_specs=[IN_SMEM, IN_VMEM],
        out_specs=(IN_VMEM,) * 4,
        name="means",
    )(core, in_vmem(told))

    def centred(rows, mean):
        out = (rows.astype(F32) - mean).astype(BF16)
        return out.reshape(part_rows, out.shape[-1])

    partial = product(centred(arrived[:, 0, :, :half], mean_half), centred(arrived[:, 1], mean_c))
    partial = partial + product(
        centred(swapped[:, 0, :, half:], mean_half), centred(swapped[:, 1], mean_c)
    )
    parcel = (partial * scale[0, 0]).astype(F16)
    pieces = exchange(parcel.reshape(NX, width, block), "x")
    summed = jnp.sum(pieces.astype(F32), axis=0)

    mine = lax.dynamic_slice_in_dim(arrived, y_idx * NZ, NZ, 0)[:, 1]
    mine = (mine.astype(F32) - mean_c).astype(BF16).astype(F32)
    norms = jnp.sum(mine * mine, axis=2).reshape(1, NZ * row_count)
    norms = jnp.pad(norms, ((0, 0), (0, LANES - NZ * row_count)))

    shift = jnp.array(SHIFT, jnp.int32)[f_idx]
    column = 2 * (z_idx % 4) + z_idx // 4
    never = -2 * block
    first = jnp.where(y_idx == column, (z_idx + shift) % NZ * width, never)
    message = pl.pallas_call(
        block_kernel,
        out_shape=pltpu.VMEM((NZ * NF, 2, LANES), F32),
        in_specs=[IN_SMEM, IN_VMEM, IN_VMEM, IN_VMEM],
        out_specs=IN_VMEM,
        name="block_stats",
    )(first.reshape(1), in_vmem(summed), in_vmem(norms), in_vmem(carried))

    seen = exchange(message, SLAB)

    def owner(z, f):
        return ((z + SHIFT[f]) % NZ) * NF + COLUMN[z]

    moves = [(z * NF + f, owner(z, f)) for z in range(NZ) for f in range(NF)]
    owned = lax.ppermute(summed.astype(F16), SLAB, moves).astype(F32)
    carried = lax.ppermute(carried, SLAB, moves)
    second = pl.pallas_call(
        functools.partial(middle_kernel, width=width),
        out_shape=pltpu.VMEM((NY, 1, LANES), F32),
        in_specs=[IN_VMEM],
        out_specs=IN_VMEM,
        name="middle_stats",
    )(in_vmem(seen))
    totals = exchange(second, "y")

    first_own = jnp.where(y_idx == f_idx, z_idx * width, never)
    shrunk, shrinkage, col_mean = pl.pallas_call(
        functools.partial(shrink_kernel, rows=total_rows, factors=factors),
        out_shape=(
            shapes((width, block), F32),
            shapes((1, 1), F32),
            shapes((NF, LANES), F32),
        ),
        in_specs=[IN_SMEM, IN_VMEM, IN_VMEM, IN_VMEM],
        out_specs=(IN_VMEM, IN_VMEM, IN_VMEM),
        name="shrink",
    )(first_own.reshape(1), in_vmem(carried), in_vmem(totals), in_vmem(owned))
    return (shrunk, shrinkage.reshape(()), col_mean.reshape(block))


def solution(mesh):
    finer = Mesh(mesh.devices.reshape(NY, NZ, NX, NC), EVERY)
    return jax.shard_map(
        shrinkage_step,
        mesh=finer,
        in_specs=(P(EVERY, None),),
        out_specs=(P(PLANE, LINE), P(), P(LINE)),
        check_vma=False,
    )
```

```python
import functools

import jax
import jax.numpy as jnp
from jax import lax
from jax.experimental import pallas as pl
from jax.experimental.pallas import tpu as pltpu
from jax.sharding import Mesh
from jax.sharding import PartitionSpec as P


PLANE = ("y", "z")
LINE = ("x", "c")
SLAB = ("z", "x", "c")
EVERY = ("y", "z", "x", "c")
F32 = jnp.float32
BF16 = jnp.bfloat16
LANES = 128
NY, NZ, NX, NC = 8, 8, 4, 2
NF = NX * NC
SHIFT = (0, 4, 1, 7, 2, 6, 3, 5)
COLUMN = tuple(2 * (z % 4) + z // 4 for z in range(NZ))
OFF, SECOND, MEANS = 64, 65, 66
F16 = jnp.float16
IN_VMEM = pl.BlockSpec(memory_space=pltpu.VMEM)
IN_SMEM = pl.BlockSpec(memory_space=pltpu.SMEM)


def deal_kernel(core_ref, x_ref, out_ref, held_ref, sems):
    block = out_ref.shape[3]

    def deal(core, b):
        order = [2 * x + core for x in range(NX)] + [2 * x + 1 - core for x in range(NX)]
        whole = x_ref[:, b * block : (b + 1) * block]
        cuts = [whole[:, k * LANES : (k + 1) * LANES] for k in range(NF)]
        for z in range(NZ):
            for place, f in enumerate(order):
                held_ref[b * NZ + z, 0, :, place * LANES : (place + 1) * LANES] = cuts[
                    (z + SHIFT[f]) % NZ
                ]

    copies = []
    for b in range(NY):
        for core in range(NC):
            pl.when(core_ref[0] == core)(functools.partial(deal, core, b))
        for z in range(NZ):
            held_ref[b * NZ + z, 1] = x_ref[:, COLUMN[z] * block : (COLUMN[z] + 1) * block]
        chunk = pl.ds(b * NZ, NZ)
        copies.append(pltpu.make_async_copy(held_ref.at[chunk], out_ref.at[chunk], sems.at[b]))
        copies[-1].start()
    for copy in copies:
        copy.wait()


def tell_kernel(core_ref, sums_ref, wide_ref, told_ref):
    far = jnp.max(wide_ref[...], axis=1, keepdims=True)
    far = 2.0 * jnp.max(far, axis=0, keepdims=True)
    lines = [
        sums_ref[part : part + 1, k * LANES : (k + 1) * LANES] for part in range(2) for k in range(NF)
    ]
    dealt = jnp.concatenate(lines[:NF], axis=0)
    swapped = jnp.concatenate(lines[NX:NF] + lines[:NX], axis=0)
    plain = jnp.where(core_ref[0] == 0, dealt, swapped)
    out = jnp.concatenate(
        [plain] + lines[NF:] + [jnp.broadcast_to(far, (8, LANES))], axis=0
    )
    for f in range(NF):
        told_ref[f] = out


def means_kernel(core_ref, told_ref, half_ref, cols_ref, carried_ref, scale_ref, *, rows, held):
    told = told_ref[...]
    sums = told[:, : 2 * NF]
    means = jnp.sum(sums, axis=0) * (1.0 / rows)
    apart = jnp.max(jnp.abs(sums * (1.0 / held) - means[None]), axis=0)

    def top(value):
        return jnp.max(jnp.max(value, axis=1, keepdims=True), axis=0, keepdims=True)

    reach = top(jnp.max(told[:, 2 * NF :], axis=0)) + top(apart)
    power = half_power(reach * reach)
    mine = jnp.where(core_ref[0] == 0, means[:NX], means[NX:NF])
    for k in range(NX):
        half_ref[:, k * LANES : (k + 1) * LANES] = mine[k : k + 1]
    for k in range(NF):
        cols_ref[:, k * LANES : (k + 1) * LANES] = means[NF + k : NF + k + 1]
    up = jnp.exp2(power)
    carried_ref[...] = jnp.concatenate(
        (means[NF:], jnp.broadcast_to(up, (8, LANES))), axis=0
    )
    scale_ref[...] = in_lane(0, jnp.exp2(-power) * (1.0 / rows), jnp.zeros((1, LANES), F32))


def add_all(value):
    return jnp.sum(jnp.sum(value, axis=1, keepdims=True), axis=0, keepdims=True)


def half_power(top):
    return jnp.clip(jnp.floor(jnp.log2(jnp.maximum(top, 1e-30))), -90.0, 90.0) - 13.0


def in_lane(k, value, row):
    slot = lax.broadcasted_iota(jnp.int32, (1, LANES), 1)
    return jnp.where(slot == k, value, row)


def block_kernel(place_ref, sum_ref, norms_ref, carried_ref, message_ref):
    width, block = sum_ref.shape
    lane = lax.broadcasted_iota(jnp.int32, (8, block), 1)
    sub = lax.broadcasted_iota(jnp.int32, (8, block), 0)
    first = place_ref[0]
    factor = jnp.concatenate([carried_ref[NF : NF + 8, :]] * (block // LANES), axis=1)
    zero = jnp.zeros((8, LANES), F32)
    off, diagonal = zero, zero
    for k in range(width // 8):
        tile = sum_ref[pl.ds(k * 8, 8), :] * factor
        hit = lane == first + k * 8 + sub
        rest = jnp.where(hit, 0.0, tile)
        kept = jnp.where(hit, tile, 0.0)
        squares = rest * rest
        for j in range(block // LANES):
            cut = slice(j * LANES, (j + 1) * LANES)
            off = off + squares[:, cut]
            diagonal = diagonal + kept[:, cut]
    own = lane[:, :LANES] % 8 == sub[:, :LANES]
    flag = jnp.where(first >= 0, 1.0, 0.0)
    mean = add_all(diagonal) / width
    apart = jnp.where(own, diagonal - mean, 0.0)
    row = in_lane(OFF, add_all(off), norms_ref[...])
    row = in_lane(SECOND, add_all(apart * apart) * flag, row)
    row = in_lane(MEANS, mean * flag, row)
    flags = in_lane(MEANS, flag, jnp.zeros((1, LANES), F32))
    message_ref[...] = jnp.broadcast_to(
        jnp.concatenate((row, flags), axis=0)[None], message_ref.shape
    )


def middle_kernel(seen_ref, message_ref, *, width):
    seen = seen_ref[...]
    slot = lax.broadcasted_iota(jnp.int32, (1, 1, LANES), 2)
    values, flags = seen[:, 0:1, :], seen[:, 1:2, :]
    norms = jnp.sum(values.reshape(NZ, NF, 1, LANES), axis=0)
    norms = jnp.where(slot < OFF, norms, 0.0)
    total = jnp.sum(values, axis=0)
    is_mean = slot == MEANS

    def lanes(row):
        return jnp.sum(row, axis=1, keepdims=True)

    mean = lanes(jnp.where(is_mean[0], total, 0.0)) / NF
    apart = jnp.where(is_mean, (values - mean[None]) * flags, 0.0)
    between = lanes(jnp.sum(apart * apart, axis=0))
    second = lanes(jnp.where(slot[0] == SECOND, total, 0.0)) + width * between
    row = jnp.zeros((1, LANES), F32)
    row = in_lane(0, lanes(jnp.sum(norms, axis=0)), row)
    row = in_lane(1, lanes(jnp.sum(norms * norms, axis=0)), row)
    row = in_lane(2, lanes(jnp.where(slot[0] == OFF, total, 0.0)), row)
    row = in_lane(3, mean, row)
    row = in_lane(4, second, row)
    message_ref[...] = jnp.broadcast_to(row[None], message_ref.shape)


def shrink_kernel(
    place_ref, carried_ref, totals_ref, owned_ref, shrunk_ref, value_ref, mean_ref, *, rows, factors
):
    width, block = shrunk_ref.shape
    first = place_ref[0]
    slot = lax.broadcasted_iota(jnp.int32, (1, LANES), 1)
    totals = totals_ref[...]
    sums = jnp.sum(totals, axis=0)

    def pick(row, k):
        return jnp.sum(jnp.where(slot == k, row, 0.0), axis=1, keepdims=True)

    mu_scale = pick(sums, 0) / (rows * factors)
    apart = totals - mu_scale[None]
    from_mu = pick(jnp.sum(apart * apart, axis=0), 3)
    spread = (pick(sums, 2) + pick(sums, 4) + block * from_mu) / factors
    norm_sq = factors * (spread + mu_scale * mu_scale)
    beta_value = (pick(sums, 1) / rows - norm_sq) / (factors * rows)
    shrinkage = beta_value / spread
    value_ref[...] = shrinkage
    mean_ref[...] = carried_ref[:NF, :]
    keep = (1.0 - shrinkage) * carried_ref[NF : NF + 1, 0:1]
    lift = shrinkage * mu_scale
    lane = lax.broadcasted_iota(jnp.int32, (8, block), 1)
    sub = lax.broadcasted_iota(jnp.int32, (8, block), 0)
    for k in range(width // 8):
        at = pl.ds(k * 8, 8)
        hit = lane == first + k * 8 + sub
        shrunk_ref[at, :] = keep * owned_ref[at, :] + jnp.where(hit, lift, 0.0)


def in_vmem(value):
    return pltpu.with_memory_space_constraint(value, pltpu.VMEM)


def flip(size):
    return [(k, k ^ 1) for k in range(size)]


def product(left, right):
    return lax.dot_general(left, right, (((0,), (0,)), ((), ())), preferred_element_type=F32)


def shrinkage_step(scenarios):
    row_count, factors = scenarios.shape
    plane = NY * NZ
    total_rows = row_count * plane * NF
    part_rows = row_count * plane
    block = factors // NY
    half, width = block // 2, block // NF
    y_idx, z_idx = lax.axis_index("y"), lax.axis_index("z")
    x_idx, c_idx = lax.axis_index("x"), lax.axis_index("c")
    f_idx = x_idx * NC + c_idx
    exchange = functools.partial(lax.all_to_all, split_axis=0, concat_axis=0, tiled=True)
    shapes = jax.ShapeDtypeStruct

    core = c_idx.reshape(1)
    packet = (plane, 2, row_count, block)
    dealt = pl.pallas_call(
        deal_kernel,
        out_shape=shapes(packet, BF16),
        in_specs=[IN_SMEM, IN_VMEM],
        out_specs=pl.BlockSpec(memory_space=pltpu.HBM),
        scratch_shapes=[pltpu.VMEM(packet, BF16), pltpu.SemaphoreType.DMA((NY,))],
        name="deal",
    )(core, scenarios)
    arrived = exchange(dealt, PLANE)

    swapped = lax.ppermute(arrived, "c", flip(NC))
    values = arrived.astype(F32)
    sums = jnp.sum(values, axis=(0, 2))
    wide = jnp.max(jnp.abs(values - values[:1, :, :1]), axis=(0, 2))
    told = pl.pallas_call(
        tell_kernel,
        out_shape=shapes((NF, 3 * NF, LANES), F32),
        in_specs=[IN_SMEM, IN_VMEM, IN_VMEM],
        out_specs=IN_VMEM,
        name="tell",
    )(core, in_vmem(sums), in_vmem(wide))
    told = exchange(told, LINE)
    mean_half, mean_c, carried, scale = pl.pallas_call(
        functools.partial(means_kernel, rows=total_rows, held=part_rows),
        out_shape=(
            pltpu.VMEM((1, half), F32),
            pltpu.VMEM((1, block), F32),
            pltpu.VMEM((2 * NF, LANES), F32),
            pltpu.VMEM((1, LANES), F32),
        ),
        in_specs=[IN_SMEM, IN_VMEM],
        out_specs=(IN_VMEM,) * 4,
        name="means",
    )(core, in_vmem(told))

    def centred(rows, mean):
        out = (rows.astype(F32) - mean).astype(BF16)
        return out.reshape(part_rows, out.shape[-1])

    partial = product(centred(arrived[:, 0, :, :half], mean_half), centred(arrived[:, 1], mean_c))
    partial = partial + product(
        centred(swapped[:, 0, :, half:], mean_half), centred(swapped[:, 1], mean_c)
    )
    parcel = (partial * scale[0, 0]).astype(F16)
    pieces = exchange(parcel.reshape(NX, width, block), "x")
    summed = jnp.sum(pieces.astype(F32), axis=0)

    mine = lax.dynamic_slice_in_dim(arrived, y_idx * NZ, NZ, 0)[:, 1]
    mine = (mine.astype(F32) - mean_c).astype(BF16).astype(F32)
    norms = jnp.sum(mine * mine, axis=2).reshape(1, NZ * row_count)
    norms = jnp.pad(norms, ((0, 0), (0, LANES - NZ * row_count)))

    shift = jnp.array(SHIFT, jnp.int32)[f_idx]
    column = 2 * (z_idx % 4) + z_idx // 4
    never = -2 * block
    first = jnp.where(y_idx == column, (z_idx + shift) % NZ * width, never)
    message = pl.pallas_call(
        block_kernel,
        out_shape=pltpu.VMEM((NZ * NF, 2, LANES), F32),
        in_specs=[IN_SMEM, IN_VMEM, IN_VMEM, IN_VMEM],
        out_specs=IN_VMEM,
        name="block_stats",
    )(first.reshape(1), in_vmem(summed), in_vmem(norms), in_vmem(carried))

    seen = exchange(message, SLAB)

    def owner(z, f):
        return ((z + SHIFT[f]) % NZ) * NF + COLUMN[z]

    moves = [(z * NF + f, owner(z, f)) for z in range(NZ) for f in range(NF)]
    owned = lax.ppermute(summed.astype(F16), SLAB, moves).astype(F32)
    carried = lax.ppermute(carried, SLAB, moves)
    second = pl.pallas_call(
        functools.partial(middle_kernel, width=width),
        out_shape=pltpu.VMEM((NY, 1, LANES), F32),
        in_specs=[IN_VMEM],
        out_specs=IN_VMEM,
        name="middle_stats",
    )(in_vmem(seen))
    totals = exchange(second, "y")

    first_own = jnp.where(y_idx == f_idx, z_idx * width, never)
    shrunk, shrinkage, col_mean = pl.pallas_call(
        functools.partial(shrink_kernel, rows=total_rows, factors=factors),
        out_shape=(
            shapes((width, block), F32),
            shapes((1, 1), F32),
            shapes((NF, LANES), F32),
        ),
        in_specs=[IN_SMEM, IN_VMEM, IN_VMEM, IN_VMEM],
        out_specs=(IN_VMEM, IN_VMEM, IN_VMEM),
        name="shrink",
    )(first_own.reshape(1), in_vmem(carried), in_vmem(totals), in_vmem(owned))
    return (shrunk, shrinkage.reshape(()), col_mean.reshape(block))


def solution(mesh):
    finer = Mesh(mesh.devices.reshape(NY, NZ, NX, NC), EVERY)
    return jax.shard_map(
        shrinkage_step,
        mesh=finer,
        in_specs=(P(EVERY, None),),
        out_specs=(P(PLANE, LINE), P(), P(LINE)),
        check_vma=False,
    )
```

```python
import functools

import jax
import jax.numpy as jnp
from jax import lax
from jax.experimental import pallas as pl
from jax.experimental.pallas import tpu as pltpu
from jax.sharding import Mesh
from jax.sharding import PartitionSpec as P


PLANE = ("y", "z")
LINE = ("x", "c")
SLAB = ("z", "x", "c")
EVERY = ("y", "z", "x", "c")
F32 = jnp.float32
BF16 = jnp.bfloat16
LANES = 128
NY, NZ, NX, NC = 8, 8, 4, 2
NF = NX * NC
SHIFT = (0, 4, 1, 7, 2, 6, 3, 5)
COLUMN = tuple(2 * (z % 4) + z // 4 for z in range(NZ))
HOLDER = tuple(COLUMN.index(block) for block in range(NZ))
OFF, SECOND, MEANS = 64, 65, 66
F16 = jnp.float16
IN_VMEM = pl.BlockSpec(memory_space=pltpu.VMEM)
IN_SMEM = pl.BlockSpec(memory_space=pltpu.SMEM)


def deal_kernel(core_ref, x_ref, out_ref):
    block = out_ref.shape[3]

    def deal(core):
        order = [2 * x + core for x in range(NX)] + [2 * x + 1 - core for x in range(NX)]
        for b in range(NY):
            whole = x_ref[:, b * block : (b + 1) * block]
            cuts = [whole[:, k * LANES : (k + 1) * LANES] for k in range(NF)]
            for z in range(NZ):
                for place, f in enumerate(order):
                    out_ref[b * NZ + z, 0, :, place * LANES : (place + 1) * LANES] = cuts[
                        (z + SHIFT[f]) % NZ
                    ]
            for y in range(NY):
                out_ref[y * NZ + HOLDER[b], 1] = whole

    for core in range(NC):
        pl.when(core_ref[0] == core)(functools.partial(deal, core))


def tell_kernel(core_ref, sums_ref, wide_ref, told_ref):
    far = jnp.max(wide_ref[...], axis=1, keepdims=True)
    far = 2.0 * jnp.max(far, axis=0, keepdims=True)
    lines = [
        sums_ref[part : part + 1, k * LANES : (k + 1) * LANES] for part in range(2) for k in range(NF)
    ]
    dealt = jnp.concatenate(lines[:NF], axis=0)
    swapped = jnp.concatenate(lines[NX:NF] + lines[:NX], axis=0)
    plain = jnp.where(core_ref[0] == 0, dealt, swapped)
    out = jnp.concatenate(
        [plain] + lines[NF:] + [jnp.broadcast_to(far, (8, LANES))], axis=0
    )
    for f in range(NF):
        told_ref[f] = out


def means_kernel(core_ref, told_ref, half_ref, cols_ref, carried_ref, scale_ref, *, rows, held):
    told = told_ref[...]
    sums = told[:, : 2 * NF]
    means = jnp.sum(sums, axis=0) * (1.0 / rows)
    apart = jnp.max(jnp.abs(sums * (1.0 / held) - means[None]), axis=0)

    def top(value):
        return jnp.max(jnp.max(value, axis=1, keepdims=True), axis=0, keepdims=True)

    reach = top(jnp.max(told[:, 2 * NF :], axis=0)) + top(apart)
    power = half_power(reach * reach)
    mine = jnp.where(core_ref[0] == 0, means[:NX], means[NX:NF])
    for k in range(NX):
        half_ref[:, k * LANES : (k + 1) * LANES] = mine[k : k + 1]
    for k in range(NF):
        cols_ref[:, k * LANES : (k + 1) * LANES] = means[NF + k : NF + k + 1]
    up = jnp.exp2(power)
    carried_ref[...] = jnp.concatenate(
        (means[NF:], jnp.broadcast_to(up, (8, LANES))), axis=0
    )
    scale_ref[...] = in_lane(0, jnp.exp2(-power) * (1.0 / rows), jnp.zeros((1, LANES), F32))


def add_all(value):
    return jnp.sum(jnp.sum(value, axis=1, keepdims=True), axis=0, keepdims=True)


def half_power(top):
    return jnp.clip(jnp.floor(jnp.log2(jnp.maximum(top, 1e-30))), -90.0, 90.0) - 13.0


def in_lane(k, value, row):
    slot = lax.broadcasted_iota(jnp.int32, (1, LANES), 1)
    return jnp.where(slot == k, value, row)


def block_kernel(place_ref, sum_ref, norms_ref, carried_ref, message_ref):
    width, block = sum_ref.shape
    lane = lax.broadcasted_iota(jnp.int32, (8, block), 1)
    sub = lax.broadcasted_iota(jnp.int32, (8, block), 0)
    first = place_ref[0]
    factor = jnp.concatenate([carried_ref[NF : NF + 8, :]] * (block // LANES), axis=1)
    zero = jnp.zeros((8, LANES), F32)
    off, diagonal = zero, zero
    for k in range(width // 8):
        tile = sum_ref[pl.ds(k * 8, 8), :] * factor
        hit = lane == first + k * 8 + sub
        rest = jnp.where(hit, 0.0, tile)
        kept = jnp.where(hit, tile, 0.0)
        squares = rest * rest
        for j in range(block // LANES):
            cut = slice(j * LANES, (j + 1) * LANES)
            off = off + squares[:, cut]
            diagonal = diagonal + kept[:, cut]
    own = lane[:, :LANES] % 8 == sub[:, :LANES]
    flag = jnp.where(first >= 0, 1.0, 0.0)
    mean = add_all(diagonal) / width
    apart = jnp.where(own, diagonal - mean, 0.0)
    row = in_lane(OFF, add_all(off), norms_ref[...])
    row = in_lane(SECOND, add_all(apart * apart) * flag, row)
    row = in_lane(MEANS, mean * flag, row)
    flags = in_lane(MEANS, flag, jnp.zeros((1, LANES), F32))
    message_ref[...] = jnp.broadcast_to(
        jnp.concatenate((row, flags), axis=0)[None], message_ref.shape
    )


def middle_kernel(seen_ref, message_ref, *, width):
    seen = seen_ref[...]
    slot = lax.broadcasted_iota(jnp.int32, (1, 1, LANES), 2)
    values, flags = seen[:, 0:1, :], seen[:, 1:2, :]
    norms = jnp.sum(values.reshape(NZ, NX, 1, LANES), axis=0)
    norms = jnp.where(slot < OFF, norms, 0.0)
    total = jnp.sum(values, axis=0)
    is_mean = slot == MEANS

    def lanes(row):
        return jnp.sum(row, axis=1, keepdims=True)

    mean = lanes(jnp.where(is_mean[0], total, 0.0)) / NX
    apart = jnp.where(is_mean, (values - mean[None]) * flags, 0.0)
    between = lanes(jnp.sum(apart * apart, axis=0))
    second = lanes(jnp.where(slot[0] == SECOND, total, 0.0)) + width * between
    row = jnp.zeros((1, LANES), F32)
    row = in_lane(0, lanes(jnp.sum(norms, axis=0)), row)
    row = in_lane(1, lanes(jnp.sum(norms * norms, axis=0)), row)
    row = in_lane(2, lanes(jnp.where(slot[0] == OFF, total, 0.0)), row)
    row = in_lane(3, mean, row)
    row = in_lane(4, second, row)
    message_ref[...] = jnp.broadcast_to(row[None], message_ref.shape)


def shrink_kernel(
    place_ref, carried_ref, totals_ref, owned_ref, shrunk_ref, value_ref, mean_ref, *, rows, factors
):
    width, block = shrunk_ref.shape
    first = place_ref[0]
    slot = lax.broadcasted_iota(jnp.int32, (1, LANES), 1)
    totals = totals_ref[...]
    sums = jnp.sum(totals, axis=0)

    def pick(row, k):
        return jnp.sum(jnp.where(slot == k, row, 0.0), axis=1, keepdims=True)

    mu_scale = pick(sums, 0) / (rows * factors)
    apart = totals - mu_scale[None]
    from_mu = pick(jnp.sum(apart * apart, axis=0), 3)
    spread = (pick(sums, 2) + pick(sums, 4) + NX * width * from_mu) / factors
    norm_sq = factors * (spread + mu_scale * mu_scale)
    beta_value = (pick(sums, 1) / rows - norm_sq) / (factors * rows)
    shrinkage = beta_value / spread
    value_ref[...] = shrinkage
    mean_ref[...] = carried_ref[:NF, :]
    keep = (1.0 - shrinkage) * carried_ref[NF : NF + 1, 0:1]
    lift = shrinkage * mu_scale
    lane = lax.broadcasted_iota(jnp.int32, (8, block), 1)
    sub = lax.broadcasted_iota(jnp.int32, (8, block), 0)
    for k in range(width // 8):
        at = pl.ds(k * 8, 8)
        hit = lane == first + k * 8 + sub
        shrunk_ref[at, :] = keep * owned_ref[at, :] + jnp.where(hit, lift, 0.0)


def in_vmem(value):
    return pltpu.with_memory_space_constraint(value, pltpu.VMEM)


def flip(size):
    return [(k, k ^ 1) for k in range(size)]


def product(left, right):
    return lax.dot_general(left, right, (((0,), (0,)), ((), ())), preferred_element_type=F32)


def shrinkage_step(scenarios):
    row_count, factors = scenarios.shape
    plane = NY * NZ
    total_rows = row_count * plane * NF
    part_rows = row_count * plane
    block = factors // NY
    half, width = block // 2, block // NF
    y_idx, z_idx = lax.axis_index("y"), lax.axis_index("z")
    x_idx, c_idx = lax.axis_index("x"), lax.axis_index("c")
    f_idx = x_idx * NC + c_idx
    exchange = functools.partial(lax.all_to_all, split_axis=0, concat_axis=0, tiled=True)
    shapes = jax.ShapeDtypeStruct

    core = c_idx.reshape(1)
    dealt = pl.pallas_call(
        deal_kernel,
        out_shape=pltpu.VMEM((plane, 2, row_count, block), BF16),
        in_specs=[IN_SMEM, IN_VMEM],
        out_specs=IN_VMEM,
        name="deal",
    )(core, scenarios)
    arrived = exchange(dealt, PLANE)

    swapped = lax.ppermute(arrived, "c", flip(NC))
    values = arrived.astype(F32)
    sums = jnp.sum(values, axis=(0, 2))
    wide = jnp.max(jnp.abs(values - values[:1, :, :1]), axis=(0, 2))
    told = pl.pallas_call(
        tell_kernel,
        out_shape=shapes((NF, 3 * NF, LANES), F32),
        in_specs=[IN_SMEM, IN_VMEM, IN_VMEM],
        out_specs=IN_VMEM,
        name="tell",
    )(core, in_vmem(sums), in_vmem(wide))
    told = exchange(told, LINE)
    mean_half, mean_c, carried, scale = pl.pallas_call(
        functools.partial(means_kernel, rows=total_rows, held=part_rows),
        out_shape=(
            pltpu.VMEM((1, half), F32),
            pltpu.VMEM((1, block), F32),
            pltpu.VMEM((2 * NF, LANES), F32),
            pltpu.VMEM((1, LANES), F32),
        ),
        in_specs=[IN_SMEM, IN_VMEM],
        out_specs=(IN_VMEM,) * 4,
        name="means",
    )(core, in_vmem(told))

    def centred(rows, mean):
        out = (rows.astype(F32) - mean).astype(BF16)
        return out.reshape(part_rows, out.shape[-1])

    partial = product(centred(arrived[:, 0, :, :half], mean_half), centred(arrived[:, 1], mean_c))
    partial = partial + product(
        centred(swapped[:, 0, :, half:], mean_half), centred(swapped[:, 1], mean_c)
    )
    parcel = (partial * scale[0, 0]).astype(F16)
    pieces = exchange(parcel.reshape(NX, width, block), "x")
    summed = jnp.sum(pieces.astype(F32), axis=0)

    mine = lax.dynamic_slice_in_dim(arrived, y_idx * NZ, NZ, 0)[:, 1]
    mine = (mine.astype(F32) - mean_c).astype(BF16).astype(F32)
    norms = jnp.sum(mine * mine, axis=2).reshape(1, NZ * row_count)
    norms = jnp.pad(norms, ((0, 0), (0, LANES - NZ * row_count)))

    shift = jnp.array(SHIFT, jnp.int32)[f_idx]
    column = 2 * (z_idx % 4) + z_idx // 4
    never = -2 * block
    first = jnp.where(y_idx == column, (z_idx + shift) % NZ * width, never)
    message = pl.pallas_call(
        block_kernel,
        out_shape=pltpu.VMEM((NZ * NX, 2, LANES), F32),
        in_specs=[IN_SMEM, IN_VMEM, IN_VMEM, IN_VMEM],
        out_specs=IN_VMEM,
        name="block_stats",
    )(first.reshape(1), in_vmem(summed), in_vmem(norms), in_vmem(carried))

    seen = exchange(message, ("z", "x"))

    def owner(z, f):
        return ((z + SHIFT[f]) % NZ) * NF + COLUMN[z]

    moves = [(z * NF + f, owner(z, f)) for z in range(NZ) for f in range(NF)]
    owned = lax.ppermute(summed.astype(F16), SLAB, moves).astype(F32)
    carried = lax.ppermute(carried, SLAB, moves)
    second = pl.pallas_call(
        functools.partial(middle_kernel, width=width),
        out_shape=pltpu.VMEM((NY * NC, 1, LANES), F32),
        in_specs=[IN_VMEM],
        out_specs=IN_VMEM,
        name="middle_stats",
    )(in_vmem(seen))
    totals = exchange(second, ("y", "c"))

    first_own = jnp.where(y_idx == f_idx, z_idx * width, never)
    shrunk, shrinkage, col_mean = pl.pallas_call(
        functools.partial(shrink_kernel, rows=total_rows, factors=factors),
        out_shape=(
            shapes((width, block), F32),
            shapes((1, 1), F32),
            shapes((NF, LANES), F32),
        ),
        in_specs=[IN_SMEM, IN_VMEM, IN_VMEM, IN_VMEM],
        out_specs=(IN_VMEM, IN_VMEM, IN_VMEM),
        name="shrink",
    )(first_own.reshape(1), in_vmem(carried), in_vmem(totals), in_vmem(owned))
    return (shrunk, shrinkage.reshape(()), col_mean.reshape(block))


def solution(mesh):
    finer = Mesh(mesh.devices.reshape(NY, NZ, NX, NC), EVERY)
    return jax.shard_map(
        shrinkage_step,
        mesh=finer,
        in_specs=(P(EVERY, None),),
        out_specs=(P(PLANE, LINE), P(), P(LINE)),
        check_vma=False,
    )
```

```python
import functools

import jax
import jax.numpy as jnp
from jax import lax
from jax.experimental import pallas as pl
from jax.experimental.pallas import tpu as pltpu
from jax.sharding import Mesh
from jax.sharding import PartitionSpec as P


PLANE = ("y", "z")
LINE = ("x", "c")
SLAB = ("z", "x", "c")
EVERY = ("y", "z", "x", "c")
F32 = jnp.float32
BF16 = jnp.bfloat16
LANES = 128
NY, NZ, NX, NC = 8, 8, 4, 2
NF = NX * NC
SHIFT = (0, 4, 1, 7, 2, 6, 3, 5)
COLUMN = tuple(2 * (z % 4) + z // 4 for z in range(NZ))
HOLDER = tuple(COLUMN.index(block) for block in range(NZ))
OFF, SECOND, MEANS = 64, 65, 66
F16 = jnp.float16
IN_VMEM = pl.BlockSpec(memory_space=pltpu.VMEM)
IN_SMEM = pl.BlockSpec(memory_space=pltpu.SMEM)


def deal_kernel(core_ref, x_ref, out_ref):
    block = out_ref.shape[3]

    def deal(core):
        order = [2 * x + core for x in range(NX)] + [2 * x + 1 - core for x in range(NX)]
        for b in range(NY):
            whole = x_ref[:, b * block : (b + 1) * block]
            cuts = [whole[:, k * LANES : (k + 1) * LANES] for k in range(NF)]
            for z in range(NZ):
                for place, f in enumerate(order):
                    out_ref[b * NZ + z, 0, :, place * LANES : (place + 1) * LANES] = cuts[
                        (z + SHIFT[f]) % NZ
                    ]
            for y in range(NY):
                out_ref[y * NZ + HOLDER[b], 1] = whole

    for core in range(NC):
        pl.when(core_ref[0] == core)(functools.partial(deal, core))


def sums_kernel(core_ref, x_ref, told_ref, sum_ref, high_ref, low_ref):
    step, steps = pl.program_id(0), pl.num_programs(0)
    _, _, _, block = x_ref.shape

    @pl.when(step == 0)
    def _():
        sum_ref[...] = jnp.zeros_like(sum_ref)
        high_ref[...] = x_ref[0].astype(F32)
        low_ref[...] = x_ref[0].astype(F32)

    for part in range(2):
        for k in range(block // LANES):
            at = slice(k * LANES, (k + 1) * LANES)
            value = x_ref[:, part, :, at]
            sum_ref[part, :, at] += jnp.sum(value.astype(F32), axis=0)
            high = jnp.max(value, axis=0).astype(F32)
            low = jnp.min(value, axis=0).astype(F32)
            high_ref[part, :, at] = jnp.maximum(high_ref[part, :, at], high)
            low_ref[part, :, at] = jnp.minimum(low_ref[part, :, at], low)

    @pl.when(step == steps - 1)
    def _():
        lines = []
        far = jnp.zeros((1, LANES), F32)
        for part in range(2):
            for k in range(block // LANES):
                at = slice(k * LANES, (k + 1) * LANES)
                lines.append(jnp.sum(sum_ref[part, :, at], axis=0, keepdims=True))
                high = jnp.max(high_ref[part, :, at], axis=0, keepdims=True)
                low = jnp.min(low_ref[part, :, at], axis=0, keepdims=True)
                far = jnp.maximum(far, high - low)
        far = jnp.max(far, axis=1, keepdims=True)
        dealt = jnp.concatenate(lines[:NF], axis=0)
        swapped = jnp.concatenate(lines[NX:NF] + lines[:NX], axis=0)
        plain = jnp.where(core_ref[0] == 0, dealt, swapped)
        out = jnp.concatenate(
            [plain] + lines[NF:] + [jnp.broadcast_to(far, (8, LANES))], axis=0
        )
        for f in range(NF):
            told_ref[f] = out


def means_kernel(core_ref, told_ref, half_ref, cols_ref, carried_ref, scale_ref, *, rows, held):
    told = told_ref[...]
    sums = told[:, : 2 * NF]
    means = jnp.sum(sums, axis=0) * (1.0 / rows)
    apart = jnp.max(jnp.abs(sums * (1.0 / held) - means[None]), axis=0)

    def top(value):
        return jnp.max(jnp.max(value, axis=1, keepdims=True), axis=0, keepdims=True)

    reach = top(jnp.max(told[:, 2 * NF :], axis=0)) + top(apart)
    power = half_power(reach * reach)
    mine = jnp.where(core_ref[0] == 0, means[:NX], means[NX:NF])
    for k in range(NX):
        half_ref[:, k * LANES : (k + 1) * LANES] = mine[k : k + 1]
    for k in range(NF):
        cols_ref[:, k * LANES : (k + 1) * LANES] = means[NF + k : NF + k + 1]
    up = jnp.exp2(power)
    carried_ref[...] = jnp.concatenate(
        (means[NF:], jnp.broadcast_to(up, (8, LANES))), axis=0
    )
    scale_ref[...] = in_lane(0, jnp.exp2(-power) * (1.0 / rows), jnp.zeros((1, LANES), F32))


def add_all(value):
    return jnp.sum(jnp.sum(value, axis=1, keepdims=True), axis=0, keepdims=True)


def half_power(top):
    return jnp.clip(jnp.floor(jnp.log2(jnp.maximum(top, 1e-30))), -90.0, 90.0) - 13.0


def in_lane(k, value, row):
    slot = lax.broadcasted_iota(jnp.int32, (1, LANES), 1)
    return jnp.where(slot == k, value, row)


def block_kernel(place_ref, sum_ref, norms_ref, carried_ref, message_ref):
    width, block = sum_ref.shape
    lane = lax.broadcasted_iota(jnp.int32, (8, block), 1)
    sub = lax.broadcasted_iota(jnp.int32, (8, block), 0)
    first = place_ref[0]
    factor = jnp.concatenate([carried_ref[NF : NF + 8, :]] * (block // LANES), axis=1)
    zero = jnp.zeros((8, LANES), F32)
    off, diagonal = zero, zero
    for k in range(width // 8):
        tile = sum_ref[pl.ds(k * 8, 8), :] * factor
        hit = lane == first + k * 8 + sub
        rest = jnp.where(hit, 0.0, tile)
        kept = jnp.where(hit, tile, 0.0)
        squares = rest * rest
        for j in range(block // LANES):
            cut = slice(j * LANES, (j + 1) * LANES)
            off = off + squares[:, cut]
            diagonal = diagonal + kept[:, cut]
    own = lane[:, :LANES] % 8 == sub[:, :LANES]
    flag = jnp.where(first >= 0, 1.0, 0.0)
    mean = add_all(diagonal) / width
    apart = jnp.where(own, diagonal - mean, 0.0)
    row = in_lane(OFF, add_all(off), norms_ref[...])
    row = in_lane(SECOND, add_all(apart * apart) * flag, row)
    row = in_lane(MEANS, mean * flag, row)
    flags = in_lane(MEANS, flag, jnp.zeros((1, LANES), F32))
    message_ref[...] = jnp.broadcast_to(
        jnp.concatenate((row, flags), axis=0)[None], message_ref.shape
    )


def middle_kernel(seen_ref, message_ref, *, width):
    seen = seen_ref[...]
    slot = lax.broadcasted_iota(jnp.int32, (1, 1, LANES), 2)
    values, flags = seen[:, 0:1, :], seen[:, 1:2, :]
    norms = jnp.sum(values.reshape(NZ, NF, 1, LANES), axis=0)
    norms = jnp.where(slot < OFF, norms, 0.0)
    total = jnp.sum(values, axis=0)
    is_mean = slot == MEANS

    def lanes(row):
        return jnp.sum(row, axis=1, keepdims=True)

    mean = lanes(jnp.where(is_mean[0], total, 0.0)) / NF
    apart = jnp.where(is_mean, (values - mean[None]) * flags, 0.0)
    between = lanes(jnp.sum(apart * apart, axis=0))
    second = lanes(jnp.where(slot[0] == SECOND, total, 0.0)) + width * between
    row = jnp.zeros((1, LANES), F32)
    row = in_lane(0, lanes(jnp.sum(norms, axis=0)), row)
    row = in_lane(1, lanes(jnp.sum(norms * norms, axis=0)), row)
    row = in_lane(2, lanes(jnp.where(slot[0] == OFF, total, 0.0)), row)
    row = in_lane(3, mean, row)
    row = in_lane(4, second, row)
    message_ref[...] = jnp.broadcast_to(row[None], message_ref.shape)


def shrink_kernel(
    place_ref, carried_ref, totals_ref, owned_ref, shrunk_ref, value_ref, mean_ref, *, rows, factors
):
    width, block = shrunk_ref.shape
    first = place_ref[0]
    slot = lax.broadcasted_iota(jnp.int32, (1, LANES), 1)
    totals = totals_ref[...]
    sums = jnp.sum(totals, axis=0)

    def pick(row, k):
        return jnp.sum(jnp.where(slot == k, row, 0.0), axis=1, keepdims=True)

    mu_scale = pick(sums, 0) / (rows * factors)
    apart = totals - mu_scale[None]
    from_mu = pick(jnp.sum(apart * apart, axis=0), 3)
    spread = (pick(sums, 2) + pick(sums, 4) + block * from_mu) / factors
    norm_sq = factors * (spread + mu_scale * mu_scale)
    beta_value = (pick(sums, 1) / rows - norm_sq) / (factors * rows)
    shrinkage = beta_value / spread
    value_ref[...] = shrinkage
    mean_ref[...] = carried_ref[:NF, :]
    keep = (1.0 - shrinkage) * carried_ref[NF : NF + 1, 0:1]
    lift = shrinkage * mu_scale
    lane = lax.broadcasted_iota(jnp.int32, (8, block), 1)
    sub = lax.broadcasted_iota(jnp.int32, (8, block), 0)
    for k in range(width // 8):
        at = pl.ds(k * 8, 8)
        hit = lane == first + k * 8 + sub
        shrunk_ref[at, :] = keep * owned_ref[at, :] + jnp.where(hit, lift, 0.0)


def in_vmem(value):
    return pltpu.with_memory_space_constraint(value, pltpu.VMEM)


def flip(size):
    return [(k, k ^ 1) for k in range(size)]


def product(left, right):
    return lax.dot_general(left, right, (((0,), (0,)), ((), ())), preferred_element_type=F32)


def shrinkage_step(scenarios):
    row_count, factors = scenarios.shape
    plane = NY * NZ
    total_rows = row_count * plane * NF
    part_rows = row_count * plane
    block = factors // NY
    half, width = block // 2, block // NF
    y_idx, z_idx = lax.axis_index("y"), lax.axis_index("z")
    x_idx, c_idx = lax.axis_index("x"), lax.axis_index("c")
    f_idx = x_idx * NC + c_idx
    exchange = functools.partial(lax.all_to_all, split_axis=0, concat_axis=0, tiled=True)
    shapes = jax.ShapeDtypeStruct

    core = c_idx.reshape(1)
    dealt = pl.pallas_call(
        deal_kernel,
        out_shape=pltpu.VMEM((plane, 2, row_count, block), BF16),
        in_specs=[IN_SMEM, IN_VMEM],
        out_specs=IN_VMEM,
        name="deal",
    )(core, scenarios)
    arrived = exchange(dealt, PLANE)

    swapped = lax.ppermute(arrived, "c", flip(NC))
    steps = 4
    packet = (plane // steps, 2, row_count, block)
    told = pl.pallas_call(
        sums_kernel,
        grid=(steps,),
        out_shape=shapes((NF, 3 * NF, LANES), F32),
        in_specs=[IN_SMEM, pl.BlockSpec(packet, lambda i: (i, 0, 0, 0))],
        out_specs=pl.BlockSpec((NF, 3 * NF, LANES), lambda i: (0, 0, 0)),
        scratch_shapes=[pltpu.VMEM((2, row_count, block), F32)] * 3,
        name="sums",
    )(core, arrived)
    told = exchange(told, LINE)
    mean_half, mean_c, carried, scale = pl.pallas_call(
        functools.partial(means_kernel, rows=total_rows, held=part_rows),
        out_shape=(
            pltpu.VMEM((1, half), F32),
            pltpu.VMEM((1, block), F32),
            pltpu.VMEM((2 * NF, LANES), F32),
            pltpu.VMEM((1, LANES), F32),
        ),
        in_specs=[IN_SMEM, IN_VMEM],
        out_specs=(IN_VMEM,) * 4,
        name="means",
    )(core, in_vmem(told))

    def centred(rows, mean):
        out = (rows.astype(F32) - mean).astype(BF16)
        return out.reshape(part_rows, out.shape[-1])

    partial = product(centred(arrived[:, 0, :, :half], mean_half), centred(arrived[:, 1], mean_c))
    partial = partial + product(
        centred(swapped[:, 0, :, half:], mean_half), centred(swapped[:, 1], mean_c)
    )
    parcel = (partial * scale[0, 0]).astype(F16)
    pieces = exchange(parcel.reshape(NX, width, block), "x")
    summed = jnp.sum(pieces.astype(F32), axis=0)

    mine = lax.dynamic_slice_in_dim(arrived, y_idx * NZ, NZ, 0)[:, 1]
    mine = (mine.astype(F32) - mean_c).astype(BF16).astype(F32)
    norms = jnp.sum(mine * mine, axis=2).reshape(1, NZ * row_count)
    norms = jnp.pad(norms, ((0, 0), (0, LANES - NZ * row_count)))

    shift = jnp.array(SHIFT, jnp.int32)[f_idx]
    column = 2 * (z_idx % 4) + z_idx // 4
    never = -2 * block
    first = jnp.where(y_idx == column, (z_idx + shift) % NZ * width, never)
    message = pl.pallas_call(
        block_kernel,
        out_shape=pltpu.VMEM((NZ * NF, 2, LANES), F32),
        in_specs=[IN_SMEM, IN_VMEM, IN_VMEM, IN_VMEM],
        out_specs=IN_VMEM,
        name="block_stats",
    )(first.reshape(1), in_vmem(summed), in_vmem(norms), in_vmem(carried))

    seen = exchange(message, SLAB)

    def owner(z, f):
        return ((z + SHIFT[f]) % NZ) * NF + COLUMN[z]

    moves = [(z * NF + f, owner(z, f)) for z in range(NZ) for f in range(NF)]
    owned = lax.ppermute(summed.astype(F16), SLAB, moves).astype(F32)
    carried = lax.ppermute(carried, SLAB, moves)
    second = pl.pallas_call(
        functools.partial(middle_kernel, width=width),
        out_shape=pltpu.VMEM((NY, 1, LANES), F32),
        in_specs=[IN_VMEM],
        out_specs=IN_VMEM,
        name="middle_stats",
    )(in_vmem(seen))
    totals = exchange(second, "y")

    first_own = jnp.where(y_idx == f_idx, z_idx * width, never)
    shrunk, shrinkage, col_mean = pl.pallas_call(
        functools.partial(shrink_kernel, rows=total_rows, factors=factors),
        out_shape=(
            shapes((width, block), F32),
            shapes((1, 1), F32),
            shapes((NF, LANES), F32),
        ),
        in_specs=[IN_SMEM, IN_VMEM, IN_VMEM, IN_VMEM],
        out_specs=(IN_VMEM, IN_VMEM, IN_VMEM),
        name="shrink",
    )(first_own.reshape(1), in_vmem(carried), in_vmem(totals), in_vmem(owned))
    return (shrunk, shrinkage.reshape(()), col_mean.reshape(block))


def solution(mesh):
    finer = Mesh(mesh.devices.reshape(NY, NZ, NX, NC), EVERY)
    return jax.shard_map(
        shrinkage_step,
        mesh=finer,
        in_specs=(P(EVERY, None),),
        out_specs=(P(PLANE, LINE), P(), P(LINE)),
        check_vma=False,
    )
```
